128 devices in a mesh: seq: 64 (over z, y, x), tp: 2 (over core).
Axes of the slice: x: 4, y: 4, z: 4, core: 2. Of those that a mesh axis runs over, the one named last changes fastest.
Arguments:
- patches: bfloat16 [16384, 1280], P('seq'), may hold values from -60 to 60
- merge_up: bfloat16 [5120, 2560], P(None, 'tp'), may hold values from -0.078125 to 0.078125
- merge_down: bfloat16 [2560, 3584], P('tp'), may hold values from -0.125 to 0.125
- dest: int32 [4096], P('seq'), may hold values from 0 to 63, as said below
- slot: int32 [4096], P('seq'), may hold values from 0 to 255, as said below
- text: bfloat16 [16384, 3584], P('seq'), may hold values from -60 to 60
- positions: int32 [3, 16384], P(None, 'seq'), may hold values from 0 to 1023
- documents: int32 [16384], P('seq'), may hold values from 0 to 7, never falling along the last dimension, each value on 1 to 8448 neighbouring positions
- w_query: bfloat16 [3584, 1792], P('seq', 'tp'), may hold values from -8 to 8
- w_key: bfloat16 [3584, 256], P('seq', 'tp'), may hold values from -8 to 8
- w_value: bfloat16 [3584, 256], P('seq', 'tp'), may hold values from -0.09375 to 0.09375
Outputs:
- layer_input: bfloat16 [16384, 3584], P('seq', 'tp')
- attended: bfloat16 [16384, 1792], P('seq', 'tp')
The draws below stay inside these ranges and needn't reach their ends.
Inputs may be any that keep to these rules, and one draw needn't show every extreme that they name: `dest`: the rows of one device name each sequence shard at most 2 times, and in every draw some sequence shard is named 2 times by the rows of every device. `slot`: no two image rows share both a sequence shard and a position. `documents`: document numbers never fall along the tokens.
All inputs are finite; a program needn't handle non-finite values.
Results may differ from the reference program's by a relative error of at most 0.0065.
Values may be sent and summed in bfloat16 or wider, within the bound.
A program may use at most 128 MiB of HBM per device.

```python
import math
import jax
import jax.numpy as jnp
import numpy as np
from jax import lax

D = 3584
VIT = 1280
MERGE_HID = 2560
HEAD = 128
QH = 14
KVH = 2
TOK_DEV = 256
TOKENS = 16384
IMG_DEV = 64
IMAGE_ROWS = 4096
PATCHES = 16384
MERGE_IN = 5120
GROUP = 7
CAP = 2
N_SEQ = 64


def scaled_field(key, row_total, col_total):
    row_scale = jnp.exp(jax.random.uniform(jax.random.fold_in(key, 21), (row_total, 1), jnp.float32, jnp.log(0.3), jnp.log(3.0)))
    col_scale = jnp.exp(jax.random.uniform(jax.random.fold_in(key, 22), (1, col_total), jnp.float32, jnp.log(0.3), jnp.log(3.0)))
    base_field = jnp.clip(jax.random.normal(jax.random.fold_in(key, 23), (row_total, col_total), jnp.float32), -6.0, 6.0)
    return base_field * row_scale * col_scale


def draw_patches(key, part):
    return scaled_field(jax.random.fold_in(key, 1), PATCHES, VIT).astype(jnp.bfloat16)


def draw_text(key, part):
    return scaled_field(jax.random.fold_in(key, 5), TOKENS, D).astype(jnp.bfloat16)


def key_base(key):
    return jnp.clip(jax.random.normal(jax.random.fold_in(key, 31), (D, KVH * HEAD), jnp.float32), -6.0, 6.0)


def draw_w_key(key, part):
    base_rows = key_base(key)
    return (base_rows * D ** (-0.5)).astype(jnp.bfloat16)


def draw_w_query(key, part):
    noise = jnp.clip(jax.random.normal(jax.random.fold_in(key, 32), (D, QH * HEAD), jnp.float32), -6.0, 6.0) * D ** (-0.5)
    return noise.astype(jnp.bfloat16)


def route_tables(key):
    candidate_total = N_SEQ * CAP
    busy_order = jax.random.permutation(jax.random.fold_in(key, 41), N_SEQ)
    busy_flag = (busy_order < max(1, N_SEQ // 8)).astype(jnp.int32)
    candidates = jnp.arange(candidate_total, dtype=jnp.int32)
    cand_dest = candidates // CAP
    noise = jax.random.randint(jax.random.fold_in(key, 42), (N_SEQ, candidate_total), 0, 2 ** 20, dtype=jnp.int32)
    scores = noise * candidate_total + candidates[None, :] + busy_flag[cand_dest][None, :] * 2 ** 29
    ignored, chosen = lax.top_k(scores, IMG_DEV)
    dest_rows = (chosen // CAP).astype(jnp.int32)
    same_dest = dest_rows[:, :, None] == dest_rows[:, None, :]
    earlier = jnp.arange(IMG_DEV)[:, None] > jnp.arange(IMG_DEV)[None, :]
    slot_order = jnp.sum(same_dest & earlier[None], axis=-1).astype(jnp.int32)
    shuffles = jax.vmap(lambda subkey: jax.random.permutation(subkey, TOK_DEV))(jax.random.split(jax.random.fold_in(key, 43), N_SEQ))
    sources = jnp.arange(N_SEQ, dtype=jnp.int32)[:, None]
    slot_rows = shuffles[dest_rows, sources * CAP + slot_order].astype(jnp.int32)
    return (dest_rows.reshape(-1), slot_rows.reshape(-1))


def draw_dest(key, part):
    return route_tables(key)[0]


def draw_slot(key, part):
    return route_tables(key)[1]


def plant(array, stream_key, smallest, high):
    dims = array.shape
    place = [jax.random.randint(jax.random.fold_in(stream_key, axis), (), 0, dims[axis]) for axis in range(len(dims))]
    array = array.at[tuple(place)].set(smallest)
    longest = dims.index(max(dims))
    place[longest] = (place[longest] + 1) % dims[longest]
    return array.at[tuple(place)].set(high)


def block_levels(key, dims, shards, least, top_value):
    level = 1.0
    for axis_at, shards_of in shards:
        draws = jax.random.uniform(jax.random.fold_in(jax.random.fold_in(key, 6), axis_at), (shards_of,), jnp.float32, least / len(shards), top_value / len(shards))
        level = level * jnp.repeat(jnp.exp(draws), dims[axis_at] // shards_of).reshape((-1,) + (1,) * (len(dims) - 1 - axis_at))
    return level


def profile(amount, total, limit, slope):
    loads = [(1 << 20) // math.isqrt(rank ** slope) + 1 for rank in range(2, amount + 1)]
    spare, given = total - limit - (amount - 1), [1] * (amount - 1)
    while spare > 0:
        movable = [i for i in range(amount - 1) if given[i] < limit]
        mass, budget = sum([loads[i] for i in movable]), spare
        for i in movable:
            addition = min(limit - given[i], max(1, budget * loads[i] // mass), spare)
            given[i] = given[i] + addition
            spare = spare - addition
    return np.array([limit] + given)


def ragged_sizes(key, amount, total, limit, lean):
    if amount == 2:
        one = jax.random.randint(key, (), max(1, total - limit), min(limit, total - 1) + 1)
        return jnp.stack([one, total - one])
    lengths = jnp.asarray(profile(amount, total, limit, lean), jnp.int32)
    twos = (amount - 1) // 2
    donor, taker = lengths[1:1 + 2 * twos:2], lengths[2:2 + 2 * twos:2]
    room = jnp.minimum(donor - 1, limit - taker)
    shifted = jax.random.randint(jax.random.fold_in(key, 1), (twos,), 0, 1 << 20) % (room + 1)
    lengths = lengths.at[1:1 + 2 * twos:2].set(donor - shifted).at[2:2 + 2 * twos:2].set(taker + shifted)
    return lengths[jax.random.permutation(jax.random.fold_in(key, 2), amount)]


def centred(key, extent, spread, most, pieces=(), kind=jnp.bfloat16):
    values = jax.random.normal(key, extent, jnp.float32) * spread
    if len(pieces) > 0:
        values = block_levels(key, extent, pieces, -0.22, 0.18) * values
    return jnp.clip(values, min=-most, max=most).astype(kind)


def setup_inputs(seed: int = 0) -> dict:
    key_list = jax.random.split(jax.random.key(seed), 12)
    return {
        "patches": draw_patches(jax.random.fold_in(key_list[11], 71), 0),
        "merge_up": centred(key_list[1], (MERGE_IN, MERGE_HID), MERGE_IN ** -0.5, 0.078125, ((1, 2),)),
        "merge_down": centred(key_list[2], (MERGE_HID, D), MERGE_HID ** -0.5, 0.125, ((0, 2),)),
        "dest": draw_dest(jax.random.fold_in(key_list[11], 71), 0),
        "slot": draw_slot(jax.random.fold_in(key_list[11], 71), 0),
        "text": draw_text(jax.random.fold_in(key_list[11], 71), 0),
        "positions": plant(jax.random.randint(key_list[6], (3, TOKENS), 0, 4 * TOK_DEV), jax.random.fold_in(key_list[6], 1), 0, (4 * TOK_DEV) - 1).astype(jnp.int32),
        "documents": jnp.searchsorted(jnp.cumsum(ragged_sizes(key_list[7], 8, TOKENS, TOKENS // 2 + TOK_DEV, 0)), jnp.arange(TOKENS), side="right").astype(jnp.int32),
        "w_query": draw_w_query(jax.random.fold_in(key_list[11], 71), 0),
        "w_key": draw_w_key(jax.random.fold_in(key_list[11], 71), 0),
        "w_value": centred(key_list[10], (D, KVH * HEAD), D ** -0.5, 0.09375, ((0, 64), (1, 2))),
    }


epsilon = 1e-06
theta_base = 1000000.0
masked_score = -1e+30

def rms_rows(values):
    floats = values.astype(jnp.float32)
    return floats * lax.rsqrt(lax.optimization_barrier(jnp.mean(floats * floats, axis=-1, keepdims=True)) + epsilon)

def rotate(vectors, positions):
    half_dim = vectors.shape[-1] // 2
    first_end = half_dim // 4
    second_end = first_end + 3 * half_dim // 8
    pair_ids = jnp.arange(half_dim, dtype=jnp.int32)
    inverse = jnp.power(theta_base, -2.0 * pair_ids.astype(jnp.float32) / (2 * half_dim))
    coords = positions.astype(jnp.float32)
    chosen = jnp.where(pair_ids[None, :] < first_end, coords[0][:, None], jnp.where(pair_ids[None, :] < second_end, coords[1][:, None], coords[2][:, None]))
    angles = chosen * inverse[None, :]
    cosine = jnp.cos(angles)[:, None, :]
    sine = jnp.sin(angles)[:, None, :]
    lower_part = vectors[..., :half_dim]
    upper_part = vectors[..., half_dim:]
    return jnp.concatenate([lower_part * cosine - upper_part * sine, upper_part * cosine + lower_part * sine], axis=-1)

def attention(roped_query, roped_key, values, documents):
    block_size = min(512, TOKENS)
    block_total = TOKENS // block_size
    query_all = roped_query.astype(jnp.float32).reshape(TOKENS, KVH, GROUP, HEAD)
    key_all = roped_key.astype(jnp.float32)
    value_all = values.astype(jnp.float32)
    score_scale = HEAD ** (-0.5)

    def one_block(block_id):
        query_block = lax.dynamic_slice_in_dim(query_all, block_id * block_size, block_size, 0)
        query_pos = block_id * block_size + jnp.arange(block_size, dtype=jnp.int32)
        query_doc = lax.dynamic_slice_in_dim(documents, block_id * block_size, block_size, 0)

        def key_step(key_id, carry):
            maxima, totals, summed = carry
            key_block = lax.dynamic_slice_in_dim(key_all, key_id * block_size, block_size, 0)
            value_block = lax.dynamic_slice_in_dim(value_all, key_id * block_size, block_size, 0)
            key_doc = lax.dynamic_slice_in_dim(documents, key_id * block_size, block_size, 0)
            key_pos = key_id * block_size + jnp.arange(block_size, dtype=jnp.int32)
            scores = jnp.einsum('qkgd,pkd->kgqp', query_block, key_block) * score_scale
            allowed = (query_pos[:, None] >= key_pos[None, :]) & (query_doc[:, None] == key_doc[None, :])
            scores = jnp.where(allowed, scores, masked_score)
            new_max = jnp.maximum(maxima, lax.optimization_barrier(jnp.max(scores, axis=-1)))
            weights = jnp.where(allowed, jnp.exp(scores - new_max[..., None]), 0.0)
            factor = jnp.exp(maxima - new_max)
            totals = totals * factor + lax.optimization_barrier(jnp.sum(weights, axis=-1))
            rounded = lax.optimization_barrier(weights.astype(jnp.bfloat16)).astype(jnp.float32)
            summed = summed * factor[..., None] + jnp.einsum('kgqp,pkd->kgqd', rounded, value_block)
            return (new_max, totals, summed)
        starting = (jnp.full((KVH, GROUP, block_size), masked_score, jnp.float32), jnp.zeros((KVH, GROUP, block_size), jnp.float32), jnp.zeros((KVH, GROUP, block_size, HEAD), jnp.float32))
        maxima, totals, summed = lax.fori_loop(0, block_id + 1, key_step, starting)
        result = summed / totals[..., None]
        return result.transpose(2, 0, 1, 3).reshape(block_size, QH * HEAD).astype(jnp.bfloat16)
    blocks = lax.map(one_block, jnp.arange(block_total, dtype=jnp.int32))
    return blocks.reshape(TOKENS, QH * HEAD)

def reference(patches, merge_up, merge_down, dest, slot, text, positions, documents, w_query, w_key, w_value):
    grouped = rms_rows(patches).astype(jnp.bfloat16).reshape(IMAGE_ROWS, MERGE_IN)
    merger_hidden = jax.nn.gelu(jnp.dot(grouped, merge_up, preferred_element_type=jnp.float32), approximate=False).astype(jnp.bfloat16)
    merged = jnp.dot(merger_hidden, merge_down, preferred_element_type=jnp.float32).astype(jnp.bfloat16)
    targets = (dest * TOK_DEV + slot).astype(jnp.int32)
    layer_input = text.at[targets].set(merged)
    normed = rms_rows(layer_input).astype(jnp.bfloat16)
    query_raw = jnp.dot(normed, w_query, preferred_element_type=jnp.float32).reshape(TOKENS, QH, HEAD)
    key_raw = jnp.dot(normed, w_key, preferred_element_type=jnp.float32).reshape(TOKENS, KVH, HEAD)
    value_raw = jnp.dot(normed, w_value, preferred_element_type=jnp.float32).reshape(TOKENS, KVH, HEAD)
    roped_query = rotate(query_raw, positions).astype(jnp.bfloat16)
    roped_key = rotate(key_raw, positions).astype(jnp.bfloat16)
    values = value_raw.astype(jnp.bfloat16)
    attended = attention(roped_query, roped_key, values, documents)
    return (layer_input, attended)
```

```python
import functools

import jax
import jax.numpy as jnp
from jax import lax
from jax.experimental import pallas as pl
from jax.experimental.pallas import tpu as pltpu
from jax.sharding import PartitionSpec as P

HEAD = 128
EPS = 1e-06
THETA = 1000000.0
MASKED = -1e30
MESH = pl.DeviceIdType.MESH
F32 = jnp.float32
BF16 = jnp.bfloat16
WINDOW = 33


def coords():
    seq = lax.axis_index("seq")
    return (seq // 16, (seq // 4) % 4, seq % 4), lax.axis_index("tp"), seq


def device(zyx, tp):
    return (zyx[0] * 16 + zyx[1] * 4 + zyx[2], tp)


def moved(zyx, dim, by):
    out = list(zyx)
    out[dim] = lax.rem(out[dim] + by + 4, 4)
    return tuple(out)


class Gather:
    def __init__(self, view, send, recv, zyx, tp):
        self.view, self.send, self.recv, self.zyx, self.tp = view, send, recv, zyx, tp
        self.orders = ((2, 1, 0), (1, 0, 2), (0, 2, 1))

    def block(self, part, phase, at, half):
        order = self.orders[part]
        index = [None, None, None]
        for place, dim in enumerate(order):
            if place < phase:
                index[dim] = pl.ds(0, 4)
            elif place == phase:
                index[dim] = at
            else:
                index[dim] = self.zyx[dim]
        if half is not None:
            dim = order[phase - 1]
            index[dim] = pl.ds(2 * half, 2)
        return self.view(part, tuple(index))

    def copy(self, part, phase, kind, incoming=False):
        dim = self.orders[part][phase]
        me = self.zyx[dim]
        up = kind < 3
        back, half = ((0, 0), (0, 1), (1, 0), (0, 1), (0, 0), (1, 1))[kind]
        if phase == 0:
            half = None
        sign = 1 if up else -1
        shift = -sign * (back + (1 if incoming else 0))
        at = lax.rem(me + shift + 4, 4)
        ref = self.block(part, phase, at, half)
        sem = (part * 3 + phase) * 6 + kind
        return pltpu.make_async_remote_copy(
            src_ref=ref,
            dst_ref=ref,
            send_sem=self.send.at[sem],
            recv_sem=self.recv.at[sem],
            device_id=device(moved(self.zyx, dim, sign), self.tp),
            device_id_type=MESH,
        )

    def kinds(self, phase):
        return (0, 3) if phase == 0 else (0, 3, 1, 4)

    def start(self, phase):
        for kind in self.kinds(phase):
            for part in range(3):
                self.copy(part, phase, kind).start()

    def forward(self, phase):
        for part in range(3):
            self.copy(part, phase, 0, True).wait_recv()
            self.copy(part, phase, 2).start()
        if phase:
            for part in range(3):
                self.copy(part, phase, 3, True).wait_recv()
                self.copy(part, phase, 5).start()

    def finish(self, phase):
        rest = (3, 2) if phase == 0 else (1, 4, 2, 5)
        for part in range(3):
            for kind in rest:
                self.copy(part, phase, kind, True).wait_recv()

    def drain(self):
        for phase in range(3):
            for part in range(3):
                for kind in (0, 3, 2) if phase == 0 else range(6):
                    self.copy(part, phase, kind).wait_send()


def iota(shape, dim):
    return lax.broadcasted_iota(jnp.int32, shape, dim)


def to_column(row):
    n = row.shape[1]
    eye = iota((n, n), 0) == iota((n, n), 1)
    return jnp.sum(jnp.where(eye, jnp.broadcast_to(row, (n, n)), 0.0), axis=1, keepdims=True)


def to_row(column):
    n = column.shape[0]
    eye = iota((n, n), 0) == iota((n, n), 1)
    return jnp.sum(jnp.where(eye, jnp.broadcast_to(column, (n, n)), 0.0), axis=0, keepdims=True)


def one_hot(flag):
    return jnp.where(flag, 1.0, 0.0).astype(BF16)


def dot(a, b):
    return jnp.dot(a, b, preferred_element_type=F32)


def front(
    patches, merge_up, merge_down, dest, slot, text, positions, documents, w_query, w_key, w_value,
    layer_out, q_out, kv_out, start_out,
    patch_v, up_v, down_v, text_v, pn, acc, disp, stage1, turned, stage2, part_f, part_s, part_r,
    merged, normed, weights, qkv,
    load, send, recv, send1, recv1, send2, recv2, send3, recv3,
):
    zyx, tp, seq = coords()
    z, y, x = zyx
    own = weights.at[z, y, x]
    loads = [
        pltpu.make_async_copy(w_query, own.at[:, pl.ds(0, 896)], load.at[0]),
        pltpu.make_async_copy(w_key, own.at[:, pl.ds(896, 128)], load.at[1]),
        pltpu.make_async_copy(w_value, own.at[:, pl.ds(1024, 128)], load.at[2]),
        pltpu.make_async_copy(patches, patch_v, load.at[3]),
    ]
    loads += [
        pltpu.make_async_copy(merge_up.at[pl.ds(1280 * p, 1280)], up_v.at[p], load.at[4 + p])
        for p in range(4)
    ]
    loads.append(pltpu.make_async_copy(merge_down, down_v, load.at[8]))
    loads.append(pltpu.make_async_copy(text, text_v, load.at[9]))
    for copy in loads:
        copy.start()

    barrier = pltpu.get_barrier_semaphore()
    partners = []
    for g in range(1, 16):
        partners.append(device(moved(moved(zyx, 0, g // 4), 1, g % 4), tp))
    for g in range(1, 4):
        partners.append(device(moved(zyx, 2, g), tp))
    partners.append((seq, 1 - tp))
    for partner in partners:
        pl.semaphore_signal(barrier, inc=1, device_id=partner, device_id_type=MESH)
    for copy in loads[:3]:
        copy.wait()
    pl.semaphore_wait(barrier, len(partners))

    def part_of(part, index):
        return weights.at[index + (slice(None), pl.ds(384 * part, 384))]

    gather = Gather(part_of, send, recv, zyx, tp)
    gather.start(0)

    loads[3].wait()
    rows = patch_v[...].astype(F32)
    scale = lax.rsqrt(jnp.mean(rows * rows, axis=1, keepdims=True) + EPS)
    scaled = (rows * scale).astype(BF16)
    o, i = iota((256, 256), 0), iota((256, 256), 1)
    pn[...] = dot(one_hot(i == 4 * (o % 64) + o // 64), scaled).astype(BF16)

    gather.forward(0)
    loads[4].wait()
    acc[...] = dot(pn[0:64], up_v[0])
    gather.finish(0)
    gather.start(1)
    for p in range(1, 4):
        loads[4 + p].wait()
        acc[...] += dot(pn[64 * p : 64 * p + 64], up_v[p])
    gather.forward(1)

    h = acc[...]
    hidden = (0.5 * h * (1.0 + lax.erf(h * 0.7071067811865476))).astype(BF16)

    dest_row = dest[...].astype(F32)
    dest_col = to_column(dest_row)
    before = (iota((64, 64), 0) < iota((64, 64), 1)) & (dest_col == dest_row)
    order = jnp.sum(jnp.where(before, 1.0, 0.0), axis=0, keepdims=True)
    place = dest_row * 2.0 + order
    chosen = one_hot(iota((128, 64), 0).astype(F32) == place)
    slot_col = to_column(slot[...].astype(F32)) + 1.0
    lane = iota((64, 128), 1)
    meta = jnp.where(lane == 0, slot_col, 0.0).astype(BF16)
    doc_col = to_column(documents[...].astype(F32))
    doc_lane = (iota((256, 128), 1) - 1).astype(F32)
    counts = jnp.sum(jnp.where(doc_col == doc_lane, 1.0, 0.0), axis=0, keepdims=True)
    routed = dot(chosen, hidden).astype(BF16)
    disp[:, :, 0:1280] = routed.reshape(16, 8, 1280)
    routed_meta = (dot(chosen, meta) + counts).astype(BF16)
    disp[:, :, 1280:1408] = routed_meta.reshape(16, 8, 128)

    me_g = z * 4 + y

    def first(g, incoming):
        away = ((4 - g // 4) % 4 * 4 + (4 - g % 4) % 4) if incoming else g
        far = moved(moved(zyx, 0, away // 4), 1, away % 4)
        at = far[0] * 4 + far[1]
        return pltpu.make_async_remote_copy(
            src_ref=disp.at[at],
            dst_ref=stage1.at[at if incoming else me_g],
            send_sem=send1.at[g],
            recv_sem=recv1.at[g],
            device_id=device(far, tp),
            device_id_type=MESH,
        )

    for g in range(1, 16):
        first(g, False).start()
    stage1[me_g] = disp[me_g]
    gather.finish(1)
    for g in range(1, 16):
        first(g, True).wait_recv()
    o, i = iota((128, 128), 0), iota((128, 128), 1)
    turn = one_hot(i == ((o % 32) // 2) * 8 + (o // 32) * 2 + o % 2)
    turned[...] = dot(turn, stage1[...].reshape(128, 1408)).astype(BF16).reshape(4, 32, 1408)

    def second(g, incoming):
        far = moved(zyx, 2, -g if incoming else g)
        return pltpu.make_async_remote_copy(
            src_ref=turned.at[far[2]],
            dst_ref=stage2.at[far[2] if incoming else x],
            send_sem=send2.at[g],
            recv_sem=recv2.at[g],
            device_id=device(far, tp),
            device_id_type=MESH,
        )

    for g in range(1, 4):
        second(g, False).start()
    gather.start(2)
    stage2[x] = turned[x]
    for g in range(1, 4):
        second(g, True).wait_recv()

    arrived = stage2[...].reshape(128, 1408)
    rows_in = arrived[:, 0:1280]
    meta_in = arrived[:, 1280:1408].astype(F32)
    loads[8].wait()

    def swap(piece):
        cols = pl.ds(896 * piece, 896)
        return pltpu.make_async_remote_copy(
            src_ref=part_s.at[:, cols],
            dst_ref=part_r.at[:, cols],
            send_sem=send3.at[piece],
            recv_sem=recv3.at[piece],
            device_id=(seq, 1 - tp),
            device_id_type=MESH,
        )

    for piece in range(4):
        cols = slice(896 * piece, 896 * piece + 896)
        partial = dot(rows_in, down_v[:, cols])
        part_f[:, cols] = partial
        part_s[:, cols] = partial.astype(BF16)
        swap(piece).start()

    totals = jnp.sum(meta_in, axis=0, keepdims=True) * 0.5
    smaller = (doc_lane < doc_col) & (doc_lane >= 0.0)
    start_col = jnp.sum(jnp.where(smaller, totals, 0.0), axis=1, keepdims=True)
    start_out[...] = jnp.broadcast_to(start_col, (256, 128))

    slot_row = to_row(meta_in[:, 0:1])
    spot = (iota((256, 128), 0) + 1).astype(F32) == slot_row
    placed = one_hot(spot)
    hit = jnp.sum(jnp.where(spot, 1.0, 0.0), axis=1, keepdims=True) > 0.5
    loads[9].wait()
    squares = jnp.zeros((256, 1), F32)
    for piece in range(4):
        cols = slice(896 * piece, 896 * piece + 896)
        swap(piece).wait_recv()
        merged[...] = (part_f[:, cols] + part_r[:, cols].astype(F32)).astype(BF16)
        layer = jnp.where(hit, dot(placed, merged[...]), text_v[:, cols].astype(F32))
        text_v[:, cols] = layer.astype(BF16)
        squares += jnp.sum(layer * layer, axis=1, keepdims=True)
    out = pltpu.make_async_copy(
        text_v.at[:, pl.ds(pl.multiple_of(tp * 1792, 128), 1792)], layer_out, load.at[10]
    )
    out.start()
    gather.forward(2)
    factor = lax.rsqrt(squares * (1.0 / 3584.0) + EPS)
    for piece in range(4):
        cols = slice(896 * piece, 896 * piece + 896)
        normed[:, cols] = (text_v[:, cols].astype(F32) * factor).astype(BF16)

    pair = iota((256, 128), 1) % 64
    inverse = jnp.exp(pair.astype(F32) * (-2.0 / 128.0 * 13.815510557964274))
    at_t = to_column(positions[0:1, :].astype(F32))
    at_h = to_column(positions[1:2, :].astype(F32))
    at_w = to_column(positions[2:3, :].astype(F32))
    coord = jnp.where(pair < 16, at_t, jnp.where(pair < 40, at_h, at_w))
    angle = coord * inverse
    cosine = jnp.cos(angle)
    sine = jnp.sin(angle)
    sine = jnp.where(iota((256, 128), 1) < 64, -sine, sine)

    gather.finish(2)

    def rotated(v):
        return v * cosine + pltpu.roll(v, 64, 1) * sine

    for piece in range(3):
        w = weights[:, :, :, :, 384 * piece : 384 * piece + 384].reshape(3584, 384)
        qkv[...] = dot(normed[...], w)
        for head in range(3):
            v = qkv[:, 128 * head : 128 * head + 128]
            at = 3 * piece + head
            if at < 7:
                q_out[at] = rotated(v).astype(BF16)
            elif at == 7:
                kv_out[:, 0:128] = rotated(v).astype(BF16)
            else:
                kv_out[:, 128:256] = v.astype(BF16)

    out.wait()
    gather.drain()
    for g in range(1, 16):
        first(g, False).wait_send()
    for g in range(1, 4):
        second(g, False).wait_send()
    for piece in range(4):
        swap(piece).wait_send()


def back(q_ref, kv_ref, start_ref, out_ref, kv, q_v, acc, top, total, load, send, recv):
    zyx, tp, seq = coords()
    z, y, x = zyx
    mine = pltpu.make_async_copy(kv_ref, kv.at[z, y, x], load.at[0])
    mine.start()
    barrier = pltpu.get_barrier_semaphore()
    for dim in range(3):
        for by in (1, -1):
            pl.semaphore_signal(
                barrier, inc=1, device_id=device(moved(zyx, dim, by), tp), device_id_type=MESH
            )
    mine.wait()
    pl.semaphore_wait(barrier, 6)
    bounds = ((0, 96), (96, 80), (176, 80))

    def part_of(part, index):
        return kv.at[index + (pl.ds(*bounds[part]), slice(None))]

    gather = Gather(part_of, send, recv, zyx, tp)
    for phase in range(3):
        gather.start(phase)
        gather.forward(phase)
        gather.finish(phase)
    gather.drain()

    scale = HEAD**-0.5
    top[...] = jnp.full(top.shape, MASKED, F32)
    total[...] = jnp.zeros(total.shape, F32)
    acc[...] = jnp.zeros(acc.shape, F32)
    last = seq // 4
    count = last - jnp.maximum(seq - WINDOW, 0) // 4 + 1
    starts = start_ref[...][:, 0:1]

    def group(step, _):
        at = last - step
        gz, gy = at // 4, at % 4
        keys = kv[gz, gy, :, :, 0:128].reshape(1024, 128)
        values = kv[gz, gy, :, :, 128:256].reshape(1024, 128)
        key_pos = (iota((256, 1024), 1) + at * 1024).astype(F32)
        query_pos = (iota((256, 1024), 0) + seq * 256).astype(F32)
        allowed = (key_pos <= query_pos) & (key_pos >= starts)

        def head(h, _):
            scores = lax.dot_general(
                q_ref[h], keys, (((1,), (1,)), ((), ())), preferred_element_type=F32
            )
            scores = jnp.where(allowed, scores * scale, MASKED)
            old = top[h]
            new = jnp.maximum(old, jnp.max(scores, axis=1, keepdims=True))
            probs = jnp.exp(scores - new[:, 0:1])
            factor = jnp.exp(old - new)
            total[h] = total[h] * factor + jnp.sum(probs, axis=1, keepdims=True)
            acc[h] = acc[h] * factor + dot(probs.astype(BF16), values)
            top[h] = new
            return 0

        lax.fori_loop(0, 7, head, 0)
        return 0

    lax.fori_loop(0, count, group, 0)
    for h in range(7):
        out_ref[:, 128 * h : 128 * h + 128] = (acc[h] / total[h]).astype(BF16)


def per_device(
    patches, merge_up, merge_down, dest, slot, text, positions, documents, w_query, w_key, w_value
):
    hbm = pl.BlockSpec(memory_space=pl.ANY)
    vmem = pl.BlockSpec(memory_space=pltpu.VMEM)
    dma = pltpu.SemaphoreType.DMA
    layer_part, q, kv, starts = pl.pallas_call(
        front,
        out_shape=(
            jax.ShapeDtypeStruct((256, 1792), BF16),
            jax.ShapeDtypeStruct((7, 256, 128), BF16),
            jax.ShapeDtypeStruct((256, 256), BF16),
            jax.ShapeDtypeStruct((256, 128), F32),
        ),
        in_specs=[hbm, hbm, hbm, vmem, vmem, hbm, vmem, vmem, hbm, hbm, hbm],
        out_specs=(hbm, vmem, vmem, vmem),
        scratch_shapes=[
            pltpu.VMEM((256, 1280), BF16),
            pltpu.VMEM((4, 1280, 1280), BF16),
            pltpu.VMEM((1280, 3584), BF16),
            pltpu.VMEM((256, 3584), BF16),
            pltpu.VMEM((256, 1280), BF16),
            pltpu.VMEM((64, 1280), F32),
            pltpu.VMEM((16, 8, 1408), BF16),
            pltpu.VMEM((16, 8, 1408), BF16),
            pltpu.VMEM((4, 32, 1408), BF16),
            pltpu.VMEM((4, 32, 1408), BF16),
            pltpu.VMEM((128, 3584), F32),
            pltpu.VMEM((128, 3584), BF16),
            pltpu.VMEM((128, 3584), BF16),
            pltpu.VMEM((128, 896), BF16),
            pltpu.VMEM((256, 3584), BF16),
            pltpu.VMEM((4, 4, 4, 56, 1152), BF16),
            pltpu.VMEM((256, 384), F32),
            dma((11,)),
            dma((54,)),
            dma((54,)),
            dma((16,)),
            dma((16,)),
            dma((4,)),
            dma((4,)),
            dma((4,)),
            dma((4,)),
        ],
        compiler_params=pltpu.CompilerParams(
            collective_id=0, has_side_effects=True, vmem_limit_bytes=60 * 1024 * 1024
        ),
        name="front",
    )(
        patches, merge_up, merge_down, dest.reshape(1, -1), slot.reshape(1, -1), text, positions,
        documents.reshape(1, -1), w_query, w_key, w_value,
    )
    attended = pl.pallas_call(
        back,
        out_shape=jax.ShapeDtypeStruct((256, 896), BF16),
        in_specs=[vmem, hbm, vmem],
        out_specs=vmem,
        scratch_shapes=[
            pltpu.VMEM((4, 4, 4, 256, 256), BF16),
            pltpu.VMEM((7, 256, 128), BF16),
            pltpu.VMEM((7, 256, 128), F32),
            pltpu.VMEM((7, 256, 128), F32),
            pltpu.VMEM((7, 256, 128), F32),
            dma((1,)),
            dma((54,)),
            dma((54,)),
        ],
        compiler_params=pltpu.CompilerParams(
            collective_id=1, has_side_effects=True, vmem_limit_bytes=60 * 1024 * 1024
        ),
        name="back",
    )(q, kv, starts)
    return (layer_part, attended)


def solution(mesh):
    in_specs = (
        P("seq", None),
        P(None, "tp"),
        P("tp", None),
        P("seq"),
        P("seq"),
        P("seq", None),
        P(None, "seq"),
        P("seq"),
        P("seq", "tp"),
        P("seq", "tp"),
        P("seq", "tp"),
    )
    out_specs = (P("seq", "tp"), P("seq", "tp"))
    return jax.shard_map(
        per_device, mesh=mesh, in_specs=in_specs, out_specs=out_specs, check_vma=False
    )
```

```python
import functools

import jax
import jax.numpy as jnp
from jax import lax
from jax.experimental import pallas as pl
from jax.experimental.pallas import tpu as pltpu
from jax.sharding import PartitionSpec as P

HEAD = 128
EPS = 1e-06
THETA = 1000000.0
MASKED = -1e30
MESH = pl.DeviceIdType.MESH
F32 = jnp.float32
BF16 = jnp.bfloat16
WINDOW = 33
UNIT = 1536
EXPONENT = HEAD**-0.5 * 1.4426950408889634


def coords():
    seq = lax.axis_index("seq")
    return (seq // 16, (seq // 4) % 4, seq % 4), lax.axis_index("tp"), seq


def device(zyx, tp):
    return (zyx[0] * 16 + zyx[1] * 4 + zyx[2], tp)


def moved(zyx, dim, by):
    out = list(zyx)
    out[dim] = lax.rem(out[dim] + by + 4, 4)
    return tuple(out)


class Gather:
    ORDERS = ((2, 1, 0), (1, 0, 2), (0, 2, 1))

    def __init__(self, weights, send, recv, zyx, tp):
        self.weights, self.send, self.recv, self.zyx, self.tp = weights, send, recv, zyx, tp

    def block(self, part, phase, at, half, early):
        order = self.ORDERS[part]
        index = [None, None, None]
        for place, dim in enumerate(order):
            if place < phase:
                index[dim] = pl.ds(0, 4)
            elif place == phase:
                index[dim] = at
            else:
                index[dim] = self.zyx[dim]
        if phase:
            index[order[phase - 1]] = pl.ds(2 * half, 2)
        columns = pl.ds(384 * part, 384)
        if phase == 2 and part < 2:
            columns = pl.ds(384 * part + 256, 128) if early else pl.ds(384 * part, 256)
        return self.weights.at[index[0], index[1], index[2], :, columns]

    def copy(self, part, phase, kind, incoming=False, early=False):
        dim = self.ORDERS[part][phase]
        me = self.zyx[dim]
        back, half = ((0, 0), (0, 1), (1, 0), (0, 1), (0, 0), (1, 1))[kind]
        step = 1 if kind < 3 else -1
        if phase == 0 and kind == 2:
            back, step = 0, 2
        shift = (1 if kind < 3 else -1) * back + (step if incoming else 0)
        at = lax.rem(me - shift + 4, 4)
        ref = self.block(part, phase, at, half, early)
        sem = 54 + part * 6 + kind if early else (part * 3 + phase) * 6 + kind
        return pltpu.make_async_remote_copy(
            src_ref=ref,
            dst_ref=ref,
            send_sem=self.send.at[sem],
            recv_sem=self.recv.at[sem],
            device_id=device(moved(self.zyx, dim, step), self.tp),
            device_id_type=MESH,
        )

    def start(self, phase, parts=(0, 1, 2), early=False):
        for kind in (0, 3, 2) if phase == 0 else (0, 3, 1, 4):
            for part in parts:
                self.copy(part, phase, kind, early=early).start()

    def forward(self, phase, parts=(0, 1, 2), early=False):
        for kind in (2, 5):
            for part in parts:
                self.copy(part, phase, kind - 2, True, early).wait_recv()
                self.copy(part, phase, kind, early=early).start()

    def finish(self, phase, parts=(0, 1, 2), early=False):
        for part in parts:
            for kind in (0, 3, 2) if phase == 0 else (1, 4, 2, 5):
                self.copy(part, phase, kind, True, early).wait_recv()

    def drain(self):
        for phase in range(3):
            for part in range(3):
                for kind in (0, 3, 2) if phase == 0 else range(6):
                    self.copy(part, phase, kind).wait_send()
        for part in range(2):
            for kind in range(6):
                self.copy(part, 2, kind, early=True).wait_send()


class Ring:
    PARTS = ((0, 48), (48, 96), (144, 112))
    ORDERS = ((2, 1, 0), (1, 0, 2), (0, 2, 1))

    def __init__(self, kv, extra, send, recv, zyx, tp, seq):
        self.kv, self.extra, self.send, self.recv = kv, extra, send, recv
        self.flat = kv.reshape(16, 4, 256, 256)
        self.zyx, self.tp, self.seq = zyx, tp, seq
        z, y, x = zyx
        self.row = 4 * z + y
        self.gives_extra = (x == 3) & (self.row < 7)
        self.takes_extra = (x == 0) & (self.row > 8)

    def base(self, source, target):
        later = (target - source + 3) // 4
        return jnp.maximum(self.zyx[0] - 2 + later, 0)

    def block(self, part, phase, at, kind):
        z, y, x = self.zyx
        tokens = pl.ds(*self.PARTS[part])
        half = (0, 1, 0, 1, 0, 1)[kind]
        if phase == 0:
            index = [z, y, x]
            index[self.ORDERS[part][0]] = at
            return self.kv.at[index[0], index[1], index[2], tokens]
        if part == 0:
            two = pl.ds(2 * half, 2)
            if phase == 1:
                return self.kv.at[z, at, two, tokens]
            return self.kv.at[at, two, :, tokens]
        if part == 1:
            if phase == 1:
                return self.kv.at[at, pl.ds(2 * half, 2), x, tokens]
            base = jnp.maximum(self.row - 8, 0)
            return self.flat.at[pl.ds(base + 5 * half, 5 - half), at, tokens]
        if phase == 1:
            base = jnp.maximum(z - 2, 0)
            return self.kv.at[pl.ds(base + 2 * half, 2 - half), y, at, tokens]
        raise NotImplementedError

    def copy(self, part, phase, kind, incoming=False):
        dim = self.ORDERS[part][phase]
        me = self.zyx[dim]
        sign = 1 if kind < 3 else -1
        back = 1 if kind in (2, 5) else 0
        if phase == 0 and kind == 2:
            sign, back = 2, 0
        at = lax.rem(me - sign * (back + (1 if incoming else 0)) + 4, 4)
        if part == 2 and phase == 2:
            to = me if incoming else lax.rem(me + sign + 4, 4)
            base = self.base(at, to)
            planes = pl.ds(base, 2)
            if back:
                planes = pl.ds(base + (1 if kind == 2 else 0), 1)
            ref = self.kv.at[planes, at, :, pl.ds(*self.PARTS[2])]
        else:
            ref = self.block(part, phase, at, kind)
        sem = (part * 3 + phase) * 6 + kind
        return pltpu.make_async_remote_copy(
            src_ref=ref,
            dst_ref=ref,
            send_sem=self.send.at[sem],
            recv_sem=self.recv.at[sem],
            device_id=device(moved(self.zyx, dim, sign), self.tp),
            device_id_type=MESH,
        )

    def own_kinds(self, part, phase):
        if phase == 0:
            return (0, 3, 2)
        if (part, phase) == (2, 2):
            return (0, 3)
        if (part, phase) == (0, 2):
            return (0, 3, 1)
        return (0, 3, 1, 4)

    def sent_on(self, phase):
        return () if phase == 0 else (2, 5)

    def start(self, phase):
        for place in range(4):
            for part in range(3):
                kinds = self.own_kinds(part, phase)
                if place < len(kinds):
                    self.copy(part, phase, kinds[place]).start()
        if phase == 2:

            @pl.when(self.gives_extra)
            def _():
                self.extra_copy(False).start()

    def wait(self, *which):
        for part, phase, kind in which:
            self.copy(part, phase, kind, True).wait_recv()

    def forward(self, phase, parts=(0, 1, 2)):
        for kind in self.sent_on(phase):
            for part in parts:
                self.wait((part, phase, kind - 2))
                self.copy(part, phase, kind).start()

    def finish(self, phase):
        for part in range(3):
            for kind in self.own_kinds(part, phase) + self.sent_on(phase):
                if phase == 0 or kind not in (0, 3):
                    self.wait((part, phase, kind))

    def drain(self):
        for phase in range(3):
            for part in range(3):
                for kind in self.own_kinds(part, phase) + self.sent_on(phase):
                    self.copy(part, phase, kind).wait_send()

        @pl.when(self.gives_extra)
        def _():
            self.extra_copy(False).wait_send()

    def extra_copy(self, incoming):
        z, y, x = self.zyx
        other = (self.seq + 64 - WINDOW if incoming else self.seq + WINDOW) % 64
        sem = 54
        return pltpu.make_async_remote_copy(
            src_ref=self.kv.at[z, y, x],
            dst_ref=self.extra,
            send_sem=self.send.at[sem],
            recv_sem=self.recv.at[sem],
            device_id=(other, self.tp),
            device_id_type=MESH,
        )

    def greet(self, barrier):
        @pl.when(self.takes_extra)
        def _():
            pl.semaphore_signal(
                barrier, inc=1, device_id=(self.seq - WINDOW, self.tp), device_id_type=MESH
            )

    def greeted(self, barrier, partners):
        @pl.when(self.gives_extra)
        def _():
            pl.semaphore_wait(barrier, partners + 1)

        @pl.when(jnp.logical_not(self.gives_extra))
        def _():
            pl.semaphore_wait(barrier, partners)

    def shard(self, part, row, col):
        begin, size = self.PARTS[part]
        return (jnp.maximum(row, 0), col, begin), (row * 4 + col) * 256 + begin, size

    def row_keys(self, at):
        return [self.shard(1, self.row - 8 + r, at) for r in range(9)]

    def plane_keys(self, at):
        y = self.zyx[1]
        own = at is y
        base = jnp.maximum(self.zyx[0] - 2, 0) if own else self.base(at, y)
        planes = range(3 if own else 2)
        return [self.shard(2, (base + p) * 4 + at, col) for p in planes for col in range(4)]

    def before_keys(self):
        z = self.zyx[0]
        return [self.shard(0, 4 * z - 4 + r, col) for r in range(4) for col in range(4)]

    def edge_keys(self):
        y = self.zyx[1]
        rows = [self.row - 8 + r + 4 * ((y + r) // 4) for r in range(5)]
        return [self.shard(0, row, col) for row in rows for col in range(4)]

    def units(self):
        z, y, x = self.zyx
        left, right = lax.rem(x + 3, 4), lax.rem(x + 1, 4)
        below, above = lax.rem(y + 3, 4), lax.rem(y + 1, 4)
        before = self.before_keys()
        stream = self.row_keys(x) + self.plane_keys(y) + before[:8] + self.row_keys(left)
        stream += self.row_keys(right) + before[8:] + self.plane_keys(below)
        stream += self.plane_keys(above) + self.row_keys(lax.rem(x + 2, 4))
        stream += self.plane_keys(lax.rem(y + 2, 4)) + self.edge_keys()
        out, room = [[]], UNIT
        for (row, col, begin), at, size in stream:
            done = 0
            while done < size:
                if room == 0:
                    out.append([])
                    room = UNIT
                take = min(size - done, room)
                out[-1].append(((row, col, begin + done), at + done, take))
                done += take
                room -= take
        return out


def iota(shape, dim):
    return lax.broadcasted_iota(jnp.int32, shape, dim)


def to_column(row):
    n = row.shape[1]
    eye = iota((n, n), 0) == iota((n, n), 1)
    return jnp.sum(jnp.where(eye, jnp.broadcast_to(row, (n, n)), 0.0), axis=1, keepdims=True)


def to_row(column):
    n = column.shape[0]
    eye = iota((n, n), 0) == iota((n, n), 1)
    return jnp.sum(jnp.where(eye, jnp.broadcast_to(column, (n, n)), 0.0), axis=0, keepdims=True)


def one_hot(flag):
    return jnp.where(flag, 1.0, 0.0).astype(BF16)


def dot(a, b):
    return jnp.dot(a, b, preferred_element_type=F32)


def whole(
    patches, merge_up, merge_down, dest, slot, text, positions, documents, w_query, w_key, w_value,
    layer_out, attended_out,
    patch_v, up_v, down_v, text_v, pn, acc, disp, stage1, turned, stage2, part_f, part_s, part_r,
    merged, normed, weights, qkv, kv, extra, bounds, query, hold, top, unit_k, unit_v,
    load, send, recv, send1, recv1, send2, recv2, send3, recv3, kv_send, kv_recv,
):
    zyx, tp, seq = coords()
    z, y, x = zyx
    own = weights.at[z, y, x]
    def columns(source, begin, size, target, sem):
        return pltpu.make_async_copy(
            source.at[:, pl.ds(begin, size)], own.at[:, pl.ds(target, size)], load.at[sem]
        )

    loads = [
        columns(w_query, 0, 256, 0, 0),
        columns(w_key, 0, 128, 256, 1),
        columns(w_query, 256, 256, 384, 2),
        pltpu.make_async_copy(patches, patch_v, load.at[3]),
    ]
    own_loads = [columns(w_value, 0, 128, 640, 11), columns(w_query, 512, 384, 768, 12)]
    own_loads += loads[:3]

    def up_part(p):
        return pltpu.make_async_copy(
            merge_up.at[pl.ds(1280 * p, 1280)], up_v.at[p], load.at[4 + p]
        )

    loads += [up_part(p) for p in range(4)]
    loads.append(pltpu.make_async_copy(merge_down, down_v, load.at[8]))
    loads.append(pltpu.make_async_copy(text, text_v, load.at[9]))
    for copy in own_loads + loads[3:]:
        copy.start()

    barrier = pltpu.get_barrier_semaphore()
    partners = []
    for g in range(1, 16):
        partners.append(device(moved(moved(zyx, 0, g // 4), 1, g % 4), tp))
    for g in range(1, 4):
        partners.append(device(moved(zyx, 2, g), tp))
    partners.append((seq, 1 - tp))
    for partner in partners:
        pl.semaphore_signal(barrier, inc=1, device_id=partner, device_id_type=MESH)
    ring = Ring(kv, extra, kv_send, kv_recv, zyx, tp, seq)
    ring.greet(barrier)
    for copy in own_loads:
        copy.wait()
    ring.greeted(barrier, len(partners))

    gather = Gather(weights, send, recv, zyx, tp)
    gather.start(0)

    loads[3].wait()
    rows = patch_v[...].astype(F32)
    scale = lax.rsqrt(jnp.mean(rows * rows, axis=1, keepdims=True) + EPS)
    scaled = (rows * scale).astype(BF16)
    o, i = iota((256, 256), 0), iota((256, 256), 1)
    pn[...] = dot(one_hot(i == 4 * (o % 64) + o // 64), scaled).astype(BF16)

    loads[4].wait()
    acc[...] = dot(pn[0:64], up_v[0])
    gather.finish(0)
    gather.start(1)

    def up_step(p, _):
        up_part(p).wait()
        acc[...] += dot(pn[pl.ds(pl.multiple_of(64 * p, 64), 64)], up_v[p])
        return 0

    lax.fori_loop(1, 4, up_step, 0)

    h = acc[...]
    hidden = (0.5 * h * (1.0 + lax.erf(h * 0.7071067811865476))).astype(BF16)

    dest_row = dest[...].astype(F32)
    dest_col = to_column(dest_row)
    before = (iota((64, 64), 0) < iota((64, 64), 1)) & (dest_col == dest_row)
    order = jnp.sum(jnp.where(before, 1.0, 0.0), axis=0, keepdims=True)
    place = dest_row * 2.0 + order
    chosen = one_hot(iota((128, 64), 0).astype(F32) == place)
    slot_col = to_column(slot[...].astype(F32)) + 1.0
    lane = iota((64, 128), 1)
    meta = jnp.where(lane == 0, slot_col, 0.0).astype(BF16)
    doc_col = to_column(documents[...].astype(F32))
    doc_lane = (iota((256, 128), 1) - 1).astype(F32)
    counts = jnp.sum(jnp.where(doc_col == doc_lane, 1.0, 0.0), axis=0, keepdims=True)
    routed = dot(chosen, hidden).astype(BF16)
    disp[:, :, 0:1280] = routed.reshape(16, 8, 1280)
    routed_meta = (dot(chosen, meta) + counts).astype(BF16)
    disp[:, :, 1280:1408] = routed_meta.reshape(16, 8, 128)

    me_g = z * 4 + y

    def first(g, incoming):
        away = ((4 - g // 4) % 4 * 4 + (4 - g % 4) % 4) if incoming else g
        far = moved(moved(zyx, 0, away // 4), 1, away % 4)
        at = far[0] * 4 + far[1]
        return pltpu.make_async_remote_copy(
            src_ref=disp.at[at],
            dst_ref=stage1.at[at if incoming else me_g],
            send_sem=send1.at[g],
            recv_sem=recv1.at[g],
            device_id=device(far, tp),
            device_id_type=MESH,
        )

    for g in range(1, 16):
        first(g, False).start()
    stage1[me_g] = disp[me_g]
    gather.forward(1)
    for g in range(1, 16):
        first(g, True).wait_recv()
    o, i = iota((128, 128), 0), iota((128, 128), 1)
    turn = one_hot(i == ((o % 32) // 2) * 8 + (o // 32) * 2 + o % 2)
    turned[...] = dot(turn, stage1[...].reshape(128, 1408)).astype(BF16).reshape(4, 32, 1408)

    def second(g, incoming):
        far = moved(zyx, 2, -g if incoming else g)
        return pltpu.make_async_remote_copy(
            src_ref=turned.at[far[2]],
            dst_ref=stage2.at[far[2] if incoming else x],
            send_sem=send2.at[g],
            recv_sem=recv2.at[g],
            device_id=device(far, tp),
            device_id_type=MESH,
        )

    for g in range(1, 4):
        second(g, False).start()
    stage2[x] = turned[x]
    gather.finish(1)
    gather.start(2, (0, 1), True)
    gather.start(2, (2,))
    gather.forward(2, (0, 1), True)
    gather.start(2, (0, 1))
    for g in range(1, 4):
        second(g, True).wait_recv()

    arrived = stage2[...].reshape(128, 1408)
    rows_in = arrived[:, 0:1280]
    meta_in = arrived[:, 1280:1408].astype(F32)
    loads[8].wait()

    def swap(piece):
        cols = pl.ds(896 * piece, 896)
        return pltpu.make_async_remote_copy(
            src_ref=part_s.at[:, cols],
            dst_ref=part_r.at[:, cols],
            send_sem=send3.at[piece],
            recv_sem=recv3.at[piece],
            device_id=(seq, 1 - tp),
            device_id_type=MESH,
        )

    for piece in range(4):
        cols = slice(896 * piece, 896 * piece + 896)
        partial = dot(rows_in, down_v[:, cols])
        part_f[:, cols] = partial
        part_s[:, cols] = partial.astype(BF16)
        swap(piece).start()

    totals = jnp.sum(meta_in, axis=0, keepdims=True) * 0.5
    smaller = (doc_lane < doc_col) & (doc_lane >= 0.0)
    start_col = jnp.sum(jnp.where(smaller, totals, 0.0), axis=1, keepdims=True)
    total_col = to_column(totals)
    sub, lane = iota((128, 128), 0) - 1, iota((128, 128), 1)
    low = jnp.sum(jnp.where((sub >= 0) & (sub < lane), total_col, 0.0), axis=0, keepdims=True)
    high = jnp.sum(jnp.where((sub >= 0) & (sub <= lane), total_col, 0.0), axis=0, keepdims=True)
    lane = iota((1, 128), 1)
    shard_low = ((lane - 8) * 256).astype(F32)
    low = jnp.where(lane < 8, low, jnp.where(lane < 72, shard_low, -1e9))
    high = jnp.where(
        lane < 8, high, jnp.where(lane < 72, shard_low + 256.0, jnp.where(lane == 72, 0.0, -1e9))
    )
    bounds[0:1, :] = low
    bounds[1:2, :] = high

    slot_row = to_row(meta_in[:, 0:1])
    spot = (iota((256, 128), 0) + 1).astype(F32) == slot_row
    placed = one_hot(spot)
    hit = jnp.sum(jnp.where(spot, 1.0, 0.0), axis=1, keepdims=True) > 0.5
    loads[9].wait()
    squares = jnp.zeros((256, 1), F32)
    for piece in range(4):
        cols = slice(896 * piece, 896 * piece + 896)
        swap(piece).wait_recv()
        merged[...] = (part_f[:, cols] + part_r[:, cols].astype(F32)).astype(BF16)
        layer = jnp.where(hit, dot(placed, merged[...]), text_v[:, cols].astype(F32))
        text_v[:, cols] = layer.astype(BF16)
        squares += jnp.sum(layer * layer, axis=1, keepdims=True)
    out = pltpu.make_async_copy(
        text_v.at[:, pl.ds(pl.multiple_of(tp * 1792, 128), 1792)], layer_out, load.at[10]
    )
    out.start()
    factor = lax.rsqrt(squares * (1.0 / 3584.0) + EPS)
    for piece in range(4):
        cols = slice(896 * piece, 896 * piece + 896)
        normed[:, cols] = (text_v[:, cols].astype(F32) * factor).astype(BF16)

    pair = iota((256, 128), 1) % 64
    inverse = jnp.exp(pair.astype(F32) * (-2.0 / 128.0 * 13.815510557964274))
    at_t = to_column(positions[0:1, :].astype(F32))
    at_h = to_column(positions[1:2, :].astype(F32))
    at_w = to_column(positions[2:3, :].astype(F32))
    coord = jnp.where(pair < 16, at_t, jnp.where(pair < 40, at_h, at_w))
    angle = coord * inverse
    cosine = jnp.cos(angle)
    sine = jnp.sin(angle)
    sine = jnp.where(iota((256, 128), 1) < 64, -sine, sine)

    def rotated(v):
        return v * cosine + pltpu.roll(v, 64, 1) * sine

    def weight(begin, size):
        return weights[:, :, :, :, begin : begin + size].reshape(3584, size)

    gather.finish(2, (0, 1), True)
    pair = jnp.concatenate([weight(256, 128), weight(640, 128)], axis=1)
    qkv[:, 0:256] = dot(normed[...], pair)
    kv[z, y, x, :, 0:128] = rotated(qkv[:, 0:128]).astype(BF16)
    kv[z, y, x, :, 128:256] = qkv[:, 128:256].astype(BF16)
    ring.start(0)
    gather.forward(2)
    wide = iota((256, 128), 1)
    shard = wide - 8
    hidden_doc = (wide < 8) & (wide.astype(F32) != doc_col)
    hidden_shard = (wide >= 8) & ((shard >= seq) | (shard < seq - WINDOW))
    veil = jnp.where(hidden_doc | hidden_shard, MASKED, 0.0).astype(BF16)
    for head in range(7):
        query[head, :, 128:256] = veil
    unit_v[:, 128:256] = jnp.ones((UNIT, 128), BF16)
    ring.finish(0)
    ring.start(1)
    ring.forward(1)
    gather.finish(2)
    for begin, size, head in ((0, 256, 0), (384, 256, 2), (768, 384, 4)):
        qkv[:, 0:size] = dot(normed[...], weight(begin, size))
        for part in range(size // 128):
            v = qkv[:, 128 * part : 128 * part + 128]
            query[head + part, :, 0:128] = rotated(v).astype(BF16)

    ones = jnp.ones((256, 128), BF16)
    keys = kv[z, y, x, :, 0:128]
    values = jnp.concatenate([kv[z, y, x, :, 128:256], ones], axis=1)
    key_at = (iota((256, 256), 1) + seq * 256).astype(F32)
    allowed = (iota((256, 256), 1) <= iota((256, 256), 0)) & (key_at >= start_col)
    for head in range(7):
        scores = lax.dot_general(
            query[head, :, 0:128], keys, (((1,), (1,)), ((), ())), preferred_element_type=F32
        )
        scores = jnp.where(allowed, scores, MASKED)
        peak = jnp.max(scores, axis=1, keepdims=True)
        top[head] = jnp.broadcast_to(peak, (256, 128))
        hold[head] = dot(jnp.exp2((scores - peak) * EXPONENT).astype(BF16), values)

    def attend(keys, values):
        def score(head):
            return lax.dot_general(
                query[head], keys, (((1,), (1,)), ((), ())), preferred_element_type=F32
            )

        scores = score(0)
        for head in range(7):
            following = score(head + 1) if head < 6 else None
            old = top[head]
            new = jnp.maximum(old, jnp.max(scores, axis=1, keepdims=True))
            probs = jnp.exp2((scores - new[:, 0:1]) * EXPONENT).astype(BF16)
            factor = jnp.exp2((old - new) * EXPONENT)
            top[head] = new
            sums = dot(probs, values)
            hold[head, :, 0:128] = hold[head, :, 0:128] * factor + sums[:, 0:128]
            hold[head, :, 128:256] = hold[head, :, 128:256] * factor + sums[:, 128:256]
            scores = following

    def marks(first_at, rows):
        at = (iota((rows, 128), 0) + first_at).astype(F32)
        return one_hot((at >= bounds[0:1, :]) & (at < bounds[1:2, :]))

    ring.finish(1)
    ring.start(2)

    def before_unit(number):
        if number == 1:
            ring.forward(2, (0, 1))
        elif number == 2:
            ring.wait((1, 2, 1), (1, 2, 4), (0, 2, 1))
            ring.forward(2, (2,))
        elif number == 4:
            ring.wait((1, 2, 2), (1, 2, 5), (2, 2, 2), (2, 2, 5))
        elif number == 5:
            ring.wait((0, 2, 2), (0, 2, 5))

    def fill(pieces):
        at = 0
        for (row, col, begin), first_at, rows in pieces:
            here = slice(at, at + rows)
            unit_k[here, 0:128] = ring.flat[row, col, begin : begin + rows, 0:128]
            unit_v[here, 0:128] = ring.flat[row, col, begin : begin + rows, 128:256]
            unit_k[here, 128:256] = marks(first_at, rows)
            at += rows

    units = ring.units()

    def unit(number, _):
        for which, pieces in enumerate(units):

            @pl.when(number == which)
            def _():
                before_unit(which)
                fill(pieces)

        attend(unit_k[...], unit_v[...])
        return 0

    lax.fori_loop(0, len(units), unit, 0)

    @pl.when(ring.takes_extra)
    def _():
        ring.extra_copy(True).wait_recv()
        keys = jnp.concatenate(
            [extra[:, 0:128], marks((seq - WINDOW) * 256, 256)], axis=1
        )
        attend(keys, jnp.concatenate([extra[:, 128:256], ones], axis=1))

    for head in range(7):
        attended_out[:, 128 * head : 128 * head + 128] = (
            hold[head, :, 0:128] / hold[head, :, 128:256]
        ).astype(BF16)

    out.wait()
    gather.drain()
    ring.drain()
    for g in range(1, 16):
        first(g, False).wait_send()
    for g in range(1, 4):
        second(g, False).wait_send()
    for piece in range(4):
        swap(piece).wait_send()


def per_device(
    patches, merge_up, merge_down, dest, slot, text, positions, documents, w_query, w_key, w_value
):
    hbm = pl.BlockSpec(memory_space=pl.ANY)
    vmem = pl.BlockSpec(memory_space=pltpu.VMEM)
    dma = pltpu.SemaphoreType.DMA
    return pl.pallas_call(
        whole,
        out_shape=(
            jax.ShapeDtypeStruct((256, 1792), BF16),
            jax.ShapeDtypeStruct((256, 896), BF16),
        ),
        in_specs=[hbm, hbm, hbm, vmem, vmem, hbm, vmem, vmem, hbm, hbm, hbm],
        out_specs=(hbm, vmem),
        scratch_shapes=[
            pltpu.VMEM((256, 1280), BF16),
            pltpu.VMEM((4, 1280, 1280), BF16),
            pltpu.VMEM((1280, 3584), BF16),
            pltpu.VMEM((256, 3584), BF16),
            pltpu.VMEM((256, 1280), BF16),
            pltpu.VMEM((64, 1280), F32),
            pltpu.VMEM((16, 8, 1408), BF16),
            pltpu.VMEM((16, 8, 1408), BF16),
            pltpu.VMEM((4, 32, 1408), BF16),
            pltpu.VMEM((4, 32, 1408), BF16),
            pltpu.VMEM((128, 3584), F32),
            pltpu.VMEM((128, 3584), BF16),
            pltpu.VMEM((128, 3584), BF16),
            pltpu.VMEM((128, 896), BF16),
            pltpu.VMEM((256, 3584), BF16),
            pltpu.VMEM((4, 4, 4, 56, 1152), BF16),
            pltpu.VMEM((256, 384), F32),
            pltpu.VMEM((4, 4, 4, 256, 256), BF16),
            pltpu.VMEM((256, 256), BF16),
            pltpu.VMEM((8, 128), F32),
            pltpu.VMEM((7, 256, 256), BF16),
            pltpu.VMEM((7, 256, 256), F32),
            pltpu.VMEM((7, 256, 128), F32),
            pltpu.VMEM((UNIT, 256), BF16),
            pltpu.VMEM((UNIT, 256), BF16),
            dma((13,)),
            dma((66,)),
            dma((66,)),
            dma((16,)),
            dma((16,)),
            dma((4,)),
            dma((4,)),
            dma((4,)),
            dma((4,)),
            dma((55,)),
            dma((55,)),
        ],
        compiler_params=pltpu.CompilerParams(
            collective_id=0, has_side_effects=True, vmem_limit_bytes=67043328
        ),
        name="whole",
    )(
        patches, merge_up, merge_down, dest.reshape(1, -1), slot.reshape(1, -1), text, positions,
        documents.reshape(1, -1), w_query, w_key, w_value,
    )


def solution(mesh):
    in_specs = (
        P("seq", None),
        P(None, "tp"),
        P("tp", None),
        P("seq"),
        P("seq"),
        P("seq", None),
        P(None, "seq"),
        P("seq"),
        P("seq", "tp"),
        P("seq", "tp"),
        P("seq", "tp"),
    )
    out_specs = (P("seq", "tp"), P("seq", "tp"))
    return jax.shard_map(
        per_device, mesh=mesh, in_specs=in_specs, out_specs=out_specs, check_vma=False
    )
```

```python
import functools

import jax
import jax.numpy as jnp
from jax import lax
from jax.experimental import pallas as pl
from jax.experimental.pallas import tpu as pltpu
from jax.sharding import PartitionSpec as P

HEAD = 128
EPS = 1e-06
THETA = 1000000.0
MASKED = -1e30
MESH = pl.DeviceIdType.MESH
F32 = jnp.float32
BF16 = jnp.bfloat16
WINDOW = 33
UNIT = 1536
EXPONENT = HEAD**-0.5 * 1.4426950408889634


def coords():
    seq = lax.axis_index("seq")
    return (seq // 16, (seq // 4) % 4, seq % 4), lax.axis_index("tp"), seq


def device(zyx, tp):
    return (zyx[0] * 16 + zyx[1] * 4 + zyx[2], tp)


def moved(zyx, dim, by):
    out = list(zyx)
    out[dim] = lax.rem(out[dim] + by + 4, 4)
    return tuple(out)


def bulk(ref, send_sem, recv_sem, seq, tp):
    return pltpu.make_async_remote_copy(
        src_ref=ref, dst_ref=ref, send_sem=send_sem, recv_sem=recv_sem,
        device_id=(seq, 1 - tp), device_id_type=MESH,
    )


class Gather:
    ORDERS = ((2, 1, 0), (1, 0, 2), (0, 2, 1))

    def __init__(self, weights, send, recv, zyx, tp, seq):
        self.weights, self.send, self.recv, self.zyx, self.tp = weights, send, recv, zyx, tp
        self.seq = seq

    def bulk(self, ref, send, recv):
        return bulk(ref, self.send.at[send], self.recv.at[recv], self.seq, self.tp)

    def make(self, part, dim, step, index, columns, phase, sem):
        index = tuple(index)
        ref = self.weights.at[index[0], index[1], index[2], :, pl.ds(*columns)]
        return pltpu.make_async_remote_copy(
            src_ref=ref,
            dst_ref=ref,
            send_sem=self.send.at[phase],
            recv_sem=self.recv.at[sem],
            device_id=device(moved(self.zyx, dim, step), self.tp),
            device_id_type=MESH,
        )

    def own(self, part, which, incoming=False):
        dim = self.ORDERS[part][0]
        step = (1, -1, 2)[which]
        index = list(self.zyx)
        index[dim] = lax.rem(index[dim] - (step if incoming else 0) + 4, 4)
        return self.make(part, dim, step, index, (384 * part, 384), 0, 0)

    def copy(self, part, phase, sign, piece, forwarded=False, incoming=False, early=False):
        order = self.ORDERS[part]
        dim = order[phase]
        index = list(self.zyx)
        if phase == 2:
            index[order[0]] = pl.ds(0, 4)
        before = order[phase - 1]
        index[before] = lax.rem(self.zyx[before] + piece, 4)
        back = sign * ((1 if forwarded else 0) + (1 if incoming else 0))
        index[dim] = lax.rem(self.zyx[dim] - back + 4, 4)
        columns = (384 * part, 384)
        if phase == 2 and part < 2:
            columns = (384 * part + 256, 128) if early else (384 * part, 256)
        group = 2 if early else phase - 1
        sem = 33 + group
        if not forwarded and sign == (1 if piece < 2 else -1):
            sem = 1 + 12 * group + 4 * part + piece
        return self.make(part, dim, sign, index, columns, phase, sem)

    def start_own(self):
        for which in range(3):
            for part in range(3):
                self.own(part, which).start()

    def finish_own(self):
        self.bulk(self.weights.at[0, 0, pl.ds(0, 3)], 0, 0).wait_recv()

    def start(self, phase, pieces, parts=(0, 1, 2), early=False):
        for piece in pieces:
            for part in parts:
                for sign in (1, -1):
                    self.copy(part, phase, sign, piece, early=early).start()

    def forward(self, phase, pieces, parts=(0, 1, 2), early=False):
        for piece in pieces:
            sign = 1 if piece < 2 else -1
            for part in parts:
                self.copy(part, phase, sign, piece, incoming=True, early=early).wait_recv()
                self.copy(part, phase, sign, piece, forwarded=True, early=early).start()

    def finish(self, phase, early=False):
        if phase == 1:
            ref = self.weights.at[0, pl.ds(0, 2)]
        else:
            ref = self.weights.at[pl.ds(0, 2), :, :, :, pl.ds(0, 256 if early else 896)]
        self.bulk(ref, phase, 35 if early else 32 + phase).wait_recv()

    def drain(self):
        self.bulk(self.weights.at[0, 0, pl.ds(0, 3)], 0, 0).wait_send()
        self.bulk(self.weights.at[0, pl.ds(0, 3)], 1, 0).wait_send()
        self.bulk(self.weights.at[pl.ds(0, 3)], 2, 0).wait_send()


class Ring:
    PARTS = ((0, 48), (48, 96), (144, 112))
    ORDERS = ((2, 1, 0), (1, 0, 2), (0, 2, 1))

    def __init__(self, kv, extra, send, recv, zyx, tp, seq):
        self.kv, self.extra, self.send, self.recv = kv, extra, send, recv
        self.flat = kv.reshape(16, 4, 256, 256)
        self.zyx, self.tp, self.seq = zyx, tp, seq
        z, y, x = zyx
        self.row = 4 * z + y
        self.gives_extra = (x == 3) & (self.row < 7)
        self.takes_extra = (x == 0) & (self.row > 8)

    def base(self, source, target):
        later = (target - source + 3) // 4
        return jnp.maximum(self.zyx[0] - 2 + later, 0)

    def block(self, part, phase, at, kind):
        z, y, x = self.zyx
        tokens = pl.ds(*self.PARTS[part])
        half = (0, 1, 0, 1, 0, 1)[kind]
        if phase == 0:
            index = [z, y, x]
            index[self.ORDERS[part][0]] = at
            return self.kv.at[index[0], index[1], index[2], tokens]
        if part == 0:
            two = pl.ds(2 * half, 2)
            if phase == 1:
                return self.kv.at[z, at, two, tokens]
            return self.kv.at[at, two, :, tokens]
        if part == 1:
            if phase == 1:
                return self.kv.at[at, pl.ds(2 * half, 2), x, tokens]
            base = jnp.maximum(self.row - 8, 0)
            return self.flat.at[pl.ds(base + 5 * half, 5 - half), at, tokens]
        if phase == 1:
            base = jnp.maximum(z - 2, 0)
            return self.kv.at[pl.ds(base + 2 * half, 2 - half), y, at, tokens]
        raise NotImplementedError

    def copy(self, part, phase, kind, incoming=False):
        dim = self.ORDERS[part][phase]
        me = self.zyx[dim]
        sign = 1 if kind < 3 else -1
        back = 1 if kind in (2, 5) else 0
        if phase == 0 and kind == 2:
            sign, back = 2, 0
        at = lax.rem(me - sign * (back + (1 if incoming else 0)) + 4, 4)
        if part == 2 and phase == 2:
            to = me if incoming else lax.rem(me + sign + 4, 4)
            base = self.base(at, to)
            planes = pl.ds(base, 2)
            if back:
                planes = pl.ds(base + (1 if kind == 2 else 0), 1)
            ref = self.kv.at[planes, at, :, pl.ds(*self.PARTS[2])]
        else:
            ref = self.block(part, phase, at, kind)
        if phase == 0:
            sends, sem = 0, 0
        elif phase == 1:
            sends, sem = 1 + part, 7 + part
            if kind in (0, 3):
                sem = 1 + 2 * part + kind // 3
        else:
            sends, sem = 4 + part, 10 + 6 * part + kind
        return pltpu.make_async_remote_copy(
            src_ref=ref,
            dst_ref=ref,
            send_sem=self.send.at[sends],
            recv_sem=self.recv.at[sem],
            device_id=device(moved(self.zyx, dim, sign), self.tp),
            device_id_type=MESH,
        )

    def own_kinds(self, part, phase):
        if phase == 0:
            return (0, 3, 2)
        if (part, phase) == (2, 2):
            return (0, 3)
        if (part, phase) == (0, 2):
            return (0, 3, 1)
        return (0, 3, 1, 4)

    def sent_on(self, phase):
        return () if phase == 0 else (2, 5)

    def start(self, phase):
        for place in range(4):
            for part in range(3):
                kinds = self.own_kinds(part, phase)
                if place < len(kinds):
                    self.copy(part, phase, kinds[place]).start()
        if phase == 2:

            @pl.when(self.gives_extra)
            def _():
                self.extra_copy(False).start()

    def wait(self, *which):
        for part, phase, kind in which:
            self.copy(part, phase, kind, True).wait_recv()

    def forward(self, phase, parts=(0, 1, 2)):
        for kind in self.sent_on(phase):
            for part in parts:
                self.wait((part, phase, kind - 2))
                self.copy(part, phase, kind).start()

    def bulk(self, rows, cols, part, send, recv):
        tokens = pl.ds(0, 256 if part is None else self.PARTS[part][1])
        ref = self.flat.at[pl.ds(0, rows), pl.ds(0, cols), tokens]
        return bulk(ref, self.send.at[send], self.recv.at[recv], self.seq, self.tp)

    def finish(self, phase):
        if phase == 0:
            self.bulk(1, 3, None, 0, 0).wait_recv()
            return
        for part in range(3):
            self.bulk(2, 3 if part == 2 else 4, part, 1 + part, 7 + part).wait_recv()

    def drain(self):
        self.bulk(1, 3, None, 0, 0).wait_send()
        for part, (rows, cols) in enumerate(((3, 4), (3, 4), (3, 3))):
            self.bulk(rows, cols, part, 1 + part, 0).wait_send()
        for part, (rows, cols) in enumerate(((10, 4), (9, 3), (6, 4))):
            self.bulk(rows, cols, part, 4 + part, 0).wait_send()

        @pl.when(self.gives_extra)
        def _():
            self.extra_copy(False).wait_send()

    def extra_copy(self, incoming):
        z, y, x = self.zyx
        other = (self.seq + 64 - WINDOW if incoming else self.seq + WINDOW) % 64
        return pltpu.make_async_remote_copy(
            src_ref=self.kv.at[z, y, x],
            dst_ref=self.extra,
            send_sem=self.send.at[7],
            recv_sem=self.recv.at[28],
            device_id=(other, self.tp),
            device_id_type=MESH,
        )

    def greet(self, barrier):
        @pl.when(self.takes_extra)
        def _():
            pl.semaphore_signal(
                barrier, inc=1, device_id=(self.seq - WINDOW, self.tp), device_id_type=MESH
            )

    def greeted(self, barrier, partners):
        @pl.when(self.gives_extra)
        def _():
            pl.semaphore_wait(barrier, partners + 1)

        @pl.when(jnp.logical_not(self.gives_extra))
        def _():
            pl.semaphore_wait(barrier, partners)

    def shard(self, part, row, col):
        begin, size = self.PARTS[part]
        return (jnp.maximum(row, 0), col, begin), (row * 4 + col) * 256 + begin, size

    def row_keys(self, at):
        return [self.shard(1, self.row - 8 + r, at) for r in range(9)]

    def plane_keys(self, at):
        y = self.zyx[1]
        own = at is y
        base = jnp.maximum(self.zyx[0] - 2, 0) if own else self.base(at, y)
        planes = range(3 if own else 2)
        return [self.shard(2, (base + p) * 4 + at, col) for p in planes for col in range(4)]

    def before_keys(self):
        z = self.zyx[0]
        return [self.shard(0, 4 * z - 4 + r, col) for r in range(4) for col in range(4)]

    def edge_keys(self):
        y = self.zyx[1]
        rows = [self.row - 8 + r + 4 * ((y + r) // 4) for r in range(5)]
        return [self.shard(0, row, col) for row in rows for col in range(4)]

    def units(self):
        z, y, x = self.zyx
        left, right = lax.rem(x + 3, 4), lax.rem(x + 1, 4)
        below, above = lax.rem(y + 3, 4), lax.rem(y + 1, 4)
        before = self.before_keys()
        stream = self.row_keys(x) + self.plane_keys(y) + before[:8] + self.row_keys(left)
        stream += self.row_keys(right) + before[8:] + self.plane_keys(below)
        stream += self.plane_keys(above) + self.row_keys(lax.rem(x + 2, 4))
        stream += self.plane_keys(lax.rem(y + 2, 4)) + self.edge_keys()
        out, room = [[]], UNIT
        for (row, col, begin), at, size in stream:
            done = 0
            while done < size:
                if room == 0:
                    out.append([])
                    room = UNIT
                take = min(size - done, room)
                out[-1].append(((row, col, begin + done), at + done, take))
                done += take
                room -= take
        return out


def iota(shape, dim):
    return lax.broadcasted_iota(jnp.int32, shape, dim)


def to_column(row):
    n = row.shape[1]
    eye = iota((n, n), 0) == iota((n, n), 1)
    return jnp.sum(jnp.where(eye, jnp.broadcast_to(row, (n, n)), 0.0), axis=1, keepdims=True)


def to_row(column):
    n = column.shape[0]
    eye = iota((n, n), 0) == iota((n, n), 1)
    return jnp.sum(jnp.where(eye, jnp.broadcast_to(column, (n, n)), 0.0), axis=0, keepdims=True)


def one_hot(flag):
    return jnp.where(flag, 1.0, 0.0).astype(BF16)


def dot(a, b):
    return jnp.dot(a, b, preferred_element_type=F32)


def whole(
    patches, merge_up, merge_down, dest, slot, text, positions, documents, w_query, w_key, w_value,
    layer_out, attended_out,
    patch_v, up_v, down_v, text_v, pn, acc, disp, stage1, turned, stage2, part_f, part_s, part_r,
    merged, normed, weights, qkv, kv, extra, bounds, query, hold, top, unit_k, unit_v,
    load, send, recv, send1, recv1, send2, recv2, send3, recv3, kv_send, kv_recv,
):
    zyx, tp, seq = coords()
    z, y, x = zyx
    own = weights.at[z, y, x]
    def columns(source, begin, size, target, sem):
        return pltpu.make_async_copy(
            source.at[:, pl.ds(begin, size)], own.at[:, pl.ds(target, size)], load.at[sem]
        )

    loads = [
        columns(w_query, 0, 256, 0, 0),
        columns(w_key, 0, 128, 256, 1),
        columns(w_query, 256, 256, 384, 2),
        pltpu.make_async_copy(patches, patch_v, load.at[3]),
    ]
    own_loads = [columns(w_value, 0, 128, 640, 11), columns(w_query, 512, 384, 768, 12)]
    own_loads += loads[:3]

    def up_part(p):
        return pltpu.make_async_copy(
            merge_up.at[pl.ds(1280 * p, 1280)], up_v.at[p], load.at[4 + p]
        )

    loads += [up_part(p) for p in range(4)]
    loads.append(pltpu.make_async_copy(merge_down, down_v, load.at[8]))
    loads.append(pltpu.make_async_copy(text, text_v, load.at[9]))
    for copy in own_loads + loads[3:]:
        copy.start()

    barrier = pltpu.get_barrier_semaphore()
    partners = []
    for g in range(1, 16):
        partners.append(device(moved(moved(zyx, 0, g // 4), 1, g % 4), tp))
    for g in range(1, 4):
        partners.append(device(moved(zyx, 2, g), tp))
    partners.append((seq, 1 - tp))
    for partner in partners:
        pl.semaphore_signal(barrier, inc=1, device_id=partner, device_id_type=MESH)
    ring = Ring(kv, extra, kv_send, kv_recv, zyx, tp, seq)
    ring.greet(barrier)
    for copy in own_loads:
        copy.wait()
    loads[3].wait()
    rows = patch_v[...].astype(F32)
    scale = lax.rsqrt(jnp.mean(rows * rows, axis=1, keepdims=True) + EPS)
    scaled = (rows * scale).astype(BF16)
    o, i = iota((256, 256), 0), iota((256, 256), 1)
    pn[...] = dot(one_hot(i == 4 * (o % 64) + o // 64), scaled).astype(BF16)

    ring.greeted(barrier, len(partners))

    gather = Gather(weights, send, recv, zyx, tp, seq)
    gather.start_own()
    gather.start(1, (0,))

    loads[4].wait()
    acc[...] = dot(pn[0:64], up_v[0])
    gather.finish_own()
    gather.start(1, (3, 1, 2))

    def up_step(p, _):
        up_part(p).wait()
        acc[...] += dot(pn[pl.ds(pl.multiple_of(64 * p, 64), 64)], up_v[p])
        return 0

    lax.fori_loop(1, 4, up_step, 0)

    h = acc[...]
    hidden = (0.5 * h * (1.0 + lax.erf(h * 0.7071067811865476))).astype(BF16)

    dest_row = dest[...].astype(F32)
    dest_col = to_column(dest_row)
    before = (iota((64, 64), 0) < iota((64, 64), 1)) & (dest_col == dest_row)
    order = jnp.sum(jnp.where(before, 1.0, 0.0), axis=0, keepdims=True)
    place = dest_row * 2.0 + order
    chosen = one_hot(iota((128, 64), 0).astype(F32) == place)
    slot_col = to_column(slot[...].astype(F32)) + 1.0
    lane = iota((64, 128), 1)
    meta = jnp.where(lane == 0, slot_col, 0.0).astype(BF16)
    doc_col = to_column(documents[...].astype(F32))
    doc_lane = (iota((256, 128), 1) - 1).astype(F32)
    counts = jnp.sum(jnp.where(doc_col == doc_lane, 1.0, 0.0), axis=0, keepdims=True)
    routed = dot(chosen, hidden).astype(BF16)
    disp[:, :, 0:1280] = routed.reshape(16, 8, 1280)
    routed_meta = (dot(chosen, meta) + counts).astype(BF16)
    disp[:, :, 1280:1408] = routed_meta.reshape(16, 8, 128)

    me_g = z * 4 + y

    def first(g):
        far = moved(moved(zyx, 0, g // 4), 1, g % 4)
        at = far[0] * 4 + far[1]
        return pltpu.make_async_remote_copy(
            src_ref=disp.at[at],
            dst_ref=stage1.at[me_g],
            send_sem=send1.at[0],
            recv_sem=recv1.at[0],
            device_id=device(far, tp),
            device_id_type=MESH,
        )

    for g in range(1, 16):
        first(g).start()
    stage1[me_g] = disp[me_g]
    gather.forward(1, (0, 3, 1, 2))
    gather.start(2, (0,), (0, 1), True)
    gather.start(2, (0,))
    bulk(stage1.at[pl.ds(0, 15)], send1.at[0], recv1.at[0], seq, tp).wait_recv()
    o, i = iota((128, 128), 0), iota((128, 128), 1)
    turn = one_hot(i == ((o % 32) // 2) * 8 + (o // 32) * 2 + o % 2)
    turned[...] = dot(turn, stage1[...].reshape(128, 1408)).astype(BF16).reshape(4, 32, 1408)

    def second(g):
        far = moved(zyx, 2, g)
        return pltpu.make_async_remote_copy(
            src_ref=turned.at[far[2]],
            dst_ref=stage2.at[x],
            send_sem=send2.at[0],
            recv_sem=recv2.at[0],
            device_id=device(far, tp),
            device_id_type=MESH,
        )

    for g in range(1, 4):
        second(g).start()
    stage2[x] = turned[x]
    gather.forward(2, (0,), (0, 1), True)
    gather.finish(1)
    gather.start(2, (3, 2, 1), (0, 1), True)
    gather.start(2, (3, 2, 1), (2,))
    gather.start(2, (3,), (0, 1))
    bulk(stage2.at[pl.ds(0, 3)], send2.at[0], recv2.at[0], seq, tp).wait_recv()
    gather.forward(2, (3, 2, 1), (0, 1), True)
    gather.start(2, (2, 1), (0, 1))

    arrived = stage2[...].reshape(128, 1408)
    rows_in = arrived[:, 0:1280]
    meta_in = arrived[:, 1280:1408].astype(F32)
    loads[8].wait()

    def swap(piece):
        cols = pl.ds(896 * piece, 896)
        return pltpu.make_async_remote_copy(
            src_ref=part_s.at[:, cols],
            dst_ref=part_r.at[:, cols],
            send_sem=send3.at[0],
            recv_sem=recv3.at[piece],
            device_id=(seq, 1 - tp),
            device_id_type=MESH,
        )

    for piece in range(4):
        cols = slice(896 * piece, 896 * piece + 896)
        partial = dot(rows_in, down_v[:, cols])
        part_f[:, cols] = partial
        part_s[:, cols] = partial.astype(BF16)
        swap(piece).start()

    totals = jnp.sum(meta_in, axis=0, keepdims=True) * 0.5
    smaller = (doc_lane < doc_col) & (doc_lane >= 0.0)
    start_col = jnp.sum(jnp.where(smaller, totals, 0.0), axis=1, keepdims=True)
    total_col = to_column(totals)
    sub, lane = iota((128, 128), 0) - 1, iota((128, 128), 1)
    low = jnp.sum(jnp.where((sub >= 0) & (sub < lane), total_col, 0.0), axis=0, keepdims=True)
    high = jnp.sum(jnp.where((sub >= 0) & (sub <= lane), total_col, 0.0), axis=0, keepdims=True)
    lane = iota((1, 128), 1)
    shard_low = ((lane - 8) * 256).astype(F32)
    low = jnp.where(lane < 8, low, jnp.where(lane < 72, shard_low, -1e9))
    high = jnp.where(
        lane < 8, high, jnp.where(lane < 72, shard_low + 256.0, jnp.where(lane == 72, 0.0, -1e9))
    )
    bounds[0:1, :] = low
    bounds[1:2, :] = high

    slot_row = to_row(meta_in[:, 0:1])
    spot = (iota((256, 128), 0) + 1).astype(F32) == slot_row
    placed = one_hot(spot)
    hit = jnp.sum(jnp.where(spot, 1.0, 0.0), axis=1, keepdims=True) > 0.5
    loads[9].wait()
    squares = jnp.zeros((256, 1), F32)
    for piece in range(4):
        cols = slice(896 * piece, 896 * piece + 896)
        swap(piece).wait_recv()
        merged[...] = (part_f[:, cols] + part_r[:, cols].astype(F32)).astype(BF16)
        layer = jnp.where(hit, dot(placed, merged[...]), text_v[:, cols].astype(F32))
        text_v[:, cols] = layer.astype(BF16)
        squares += jnp.sum(layer * layer, axis=1, keepdims=True)
    out = pltpu.make_async_copy(
        text_v.at[:, pl.ds(pl.multiple_of(tp * 1792, 128), 1792)], layer_out, load.at[10]
    )
    out.start()
    factor = lax.rsqrt(squares * (1.0 / 3584.0) + EPS)
    for piece in range(4):
        cols = slice(896 * piece, 896 * piece + 896)
        normed[:, cols] = (text_v[:, cols].astype(F32) * factor).astype(BF16)

    pair = iota((256, 128), 1) % 64
    inverse = jnp.exp(pair.astype(F32) * (-2.0 / 128.0 * 13.815510557964274))
    at_t = to_column(positions[0:1, :].astype(F32))
    at_h = to_column(positions[1:2, :].astype(F32))
    at_w = to_column(positions[2:3, :].astype(F32))
    coord = jnp.where(pair < 16, at_t, jnp.where(pair < 40, at_h, at_w))
    angle = coord * inverse
    cosine = jnp.cos(angle)
    sine = jnp.sin(angle)
    sine = jnp.where(iota((256, 128), 1) < 64, -sine, sine)

    def rotated(v):
        return v * cosine + pltpu.roll(v, 64, 1) * sine

    def weight(begin, size):
        return weights[:, :, :, :, begin : begin + size].reshape(3584, size)

    gather.finish(2, True)
    pair = jnp.concatenate([weight(256, 128), weight(640, 128)], axis=1)
    qkv[:, 0:256] = dot(normed[...], pair)
    kv[z, y, x, :, 0:128] = rotated(qkv[:, 0:128]).astype(BF16)
    kv[z, y, x, :, 128:256] = qkv[:, 128:256].astype(BF16)
    ring.start(0)
    gather.forward(2, (0, 3, 2, 1))
    wide = iota((256, 128), 1)
    shard = wide - 8
    hidden_doc = (wide < 8) & (wide.astype(F32) != doc_col)
    hidden_shard = (wide >= 8) & ((shard >= seq) | (shard < seq - WINDOW))
    veil = jnp.where(hidden_doc | hidden_shard, MASKED, 0.0).astype(BF16)
    for head in range(7):
        query[head, :, 128:256] = veil
    unit_v[:, 128:256] = jnp.ones((UNIT, 128), BF16)
    ring.finish(0)
    ring.start(1)
    ring.forward(1)
    gather.finish(2)
    for begin, size, head in ((0, 256, 0), (384, 256, 2), (768, 384, 4)):
        qkv[:, 0:size] = dot(normed[...], weight(begin, size))
        for part in range(size // 128):
            v = qkv[:, 128 * part : 128 * part + 128]
            query[head + part, :, 0:128] = rotated(v).astype(BF16)

    ones = jnp.ones((256, 128), BF16)
    keys = kv[z, y, x, :, 0:128]
    values = jnp.concatenate([kv[z, y, x, :, 128:256], ones], axis=1)
    key_at = (iota((256, 256), 1) + seq * 256).astype(F32)
    allowed = (iota((256, 256), 1) <= iota((256, 256), 0)) & (key_at >= start_col)
    for head in range(7):
        scores = lax.dot_general(
            query[head, :, 0:128], keys, (((1,), (1,)), ((), ())), preferred_element_type=F32
        )
        scores = jnp.where(allowed, scores, MASKED)
        peak = jnp.max(scores, axis=1, keepdims=True)
        top[head] = jnp.broadcast_to(peak, (256, 128))
        hold[head] = dot(jnp.exp2((scores - peak) * EXPONENT).astype(BF16), values)

    def attend(keys, values):
        def score(head):
            return lax.dot_general(
                query[head], keys, (((1,), (1,)), ((), ())), preferred_element_type=F32
            )

        scores = score(0)
        for head in range(7):
            following = score(head + 1) if head < 6 else None
            old = top[head]
            new = jnp.maximum(old, jnp.max(scores, axis=1, keepdims=True))
            probs = jnp.exp2((scores - new[:, 0:1]) * EXPONENT).astype(BF16)
            factor = jnp.exp2((old - new) * EXPONENT)
            top[head] = new
            sums = dot(probs, values)
            hold[head, :, 0:128] = hold[head, :, 0:128] * factor + sums[:, 0:128]
            hold[head, :, 128:256] = hold[head, :, 128:256] * factor + sums[:, 128:256]
            scores = following

    def marks(first_at, rows):
        at = (iota((rows, 128), 0) + first_at).astype(F32)
        return one_hot((at >= bounds[0:1, :]) & (at < bounds[1:2, :]))

    ring.finish(1)
    ring.start(2)

    def before_unit(number):
        if number == 1:
            ring.forward(2, (0, 1))
        elif number == 2:
            ring.wait((1, 2, 1), (1, 2, 4), (0, 2, 1))
            ring.forward(2, (2,))
        elif number == 4:
            ring.wait((1, 2, 2), (1, 2, 5), (2, 2, 2), (2, 2, 5))
        elif number == 5:
            ring.wait((0, 2, 2), (0, 2, 5))

    def fill(pieces):
        at = 0
        for (row, col, begin), first_at, rows in pieces:
            here = slice(at, at + rows)
            unit_k[here, 0:128] = ring.flat[row, col, begin : begin + rows, 0:128]
            unit_v[here, 0:128] = ring.flat[row, col, begin : begin + rows, 128:256]
            unit_k[here, 128:256] = marks(first_at, rows)
            at += rows

    units = ring.units()

    def unit(number, _):
        for which, pieces in enumerate(units):

            @pl.when(number == which)
            def _():
                before_unit(which)
                fill(pieces)

        attend(unit_k[...], unit_v[...])
        return 0

    lax.fori_loop(0, len(units), unit, 0)

    @pl.when(ring.takes_extra)
    def _():
        ring.extra_copy(True).wait_recv()
        keys = jnp.concatenate(
            [extra[:, 0:128], marks((seq - WINDOW) * 256, 256)], axis=1
        )
        attend(keys, jnp.concatenate([extra[:, 128:256], ones], axis=1))

    for head in range(7):
        attended_out[:, 128 * head : 128 * head + 128] = (
            hold[head, :, 0:128] / hold[head, :, 128:256]
        ).astype(BF16)

    out.wait()
    gather.drain()
    ring.drain()
    bulk(stage1.at[pl.ds(0, 15)], send1.at[0], recv1.at[0], seq, tp).wait_send()
    bulk(stage2.at[pl.ds(0, 3)], send2.at[0], recv2.at[0], seq, tp).wait_send()
    bulk(part_s, send3.at[0], recv3.at[0], seq, tp).wait_send()


def hand_over(layer, attended, layer_out, attended_out, layer_v, attended_v, into, out):
    moves = []
    for n in range(4):
        moves.append((layer, layer_v, layer_out, pl.ds(64 * n, 64)))
    for n in range(2):
        moves.append((attended, attended_v, attended_out, pl.ds(128 * n, 128)))
    first = [
        pltpu.make_async_copy(a.at[rows], b.at[rows], into.at[n])
        for n, (a, b, _, rows) in enumerate(moves)
    ]
    then = [
        pltpu.make_async_copy(b.at[rows], c.at[rows], out.at[n])
        for n, (_, b, c, rows) in enumerate(moves)
    ]
    for copy in first:
        copy.start()
    for arrives, leaves in zip(first, then):
        arrives.wait()
        leaves.start()
    for copy in then:
        copy.wait()


def per_device(
    patches, merge_up, merge_down, dest, slot, text, positions, documents, w_query, w_key, w_value
):
    hbm = pl.BlockSpec(memory_space=pl.ANY)
    vmem = pl.BlockSpec(memory_space=pltpu.VMEM)
    dma = pltpu.SemaphoreType.DMA
    layer_part, attended = pl.pallas_call(
        whole,
        out_shape=(
            jax.ShapeDtypeStruct((256, 1792), BF16),
            jax.ShapeDtypeStruct((256, 896), BF16),
        ),
        in_specs=[hbm, hbm, hbm, vmem, vmem, hbm, vmem, vmem, hbm, hbm, hbm],
        out_specs=(hbm, vmem),
        scratch_shapes=[
            pltpu.VMEM((256, 1280), BF16),
            pltpu.VMEM((4, 1280, 1280), BF16),
            pltpu.VMEM((1280, 3584), BF16),
            pltpu.VMEM((256, 3584), BF16),
            pltpu.VMEM((256, 1280), BF16),
            pltpu.VMEM((64, 1280), F32),
            pltpu.VMEM((16, 8, 1408), BF16),
            pltpu.VMEM((16, 8, 1408), BF16),
            pltpu.VMEM((4, 32, 1408), BF16),
            pltpu.VMEM((4, 32, 1408), BF16),
            pltpu.VMEM((128, 3584), F32),
            pltpu.VMEM((128, 3584), BF16),
            pltpu.VMEM((128, 3584), BF16),
            pltpu.VMEM((128, 896), BF16),
            pltpu.VMEM((256, 3584), BF16),
            pltpu.VMEM((4, 4, 4, 56, 1152), BF16),
            pltpu.VMEM((256, 384), F32),
            pltpu.VMEM((4, 4, 4, 256, 256), BF16),
            pltpu.VMEM((256, 256), BF16),
            pltpu.VMEM((8, 128), F32),
            pltpu.VMEM((7, 256, 256), BF16),
            pltpu.VMEM((7, 256, 256), F32),
            pltpu.VMEM((7, 256, 128), F32),
            pltpu.VMEM((UNIT, 256), BF16),
            pltpu.VMEM((UNIT, 256), BF16),
            dma((13,)),
            dma((3,)),
            dma((36,)),
            dma((1,)),
            dma((1,)),
            dma((1,)),
            dma((1,)),
            dma((1,)),
            dma((4,)),
            dma((8,)),
            dma((29,)),
        ],
        compiler_params=pltpu.CompilerParams(
            collective_id=0, has_side_effects=True, vmem_limit_bytes=67043328
        ),
        name="whole",
    )(
        patches, merge_up, merge_down, dest.reshape(1, -1), slot.reshape(1, -1), text, positions,
        documents.reshape(1, -1), w_query, w_key, w_value,
    )
    return pl.pallas_call(
        hand_over,
        out_shape=(
            jax.ShapeDtypeStruct((256, 1792), BF16),
            jax.ShapeDtypeStruct((256, 896), BF16),
        ),
        in_specs=[hbm, hbm],
        out_specs=(hbm, hbm),
        scratch_shapes=[
            pltpu.VMEM((256, 1792), BF16),
            pltpu.VMEM((256, 896), BF16),
            dma((6,)),
            dma((6,)),
        ],
        name="hand_over",
    )(layer_part, attended)


def solution(mesh):
    in_specs = (
        P("seq", None),
        P(None, "tp"),
        P("tp", None),
        P("seq"),
        P("seq"),
        P("seq", None),
        P(None, "seq"),
        P("seq"),
        P("seq", "tp"),
        P("seq", "tp"),
        P("seq", "tp"),
    )
    out_specs = (P("seq", "tp"), P("seq", "tp"))
    return jax.shard_map(
        per_device, mesh=mesh, in_specs=in_specs, out_specs=out_specs, check_vma=False
    )
```

```python
import functools

import jax
import jax.numpy as jnp
from jax import lax
from jax.experimental import pallas as pl
from jax.experimental.pallas import tpu as pltpu
from jax.sharding import PartitionSpec as P

HEAD = 128
EPS = 1e-06
THETA = 1000000.0
MASKED = -1e30
MESH = pl.DeviceIdType.MESH
F32 = jnp.float32
BF16 = jnp.bfloat16
WINDOW = 33
UNIT = 1536
EXPONENT = HEAD**-0.5 * 1.4426950408889634


def coords():
    seq = lax.axis_index("seq")
    return (seq // 16, (seq // 4) % 4, seq % 4), lax.axis_index("tp"), seq


def device(zyx, tp):
    return (zyx[0] * 16 + zyx[1] * 4 + zyx[2], tp)


def moved(zyx, dim, by):
    out = list(zyx)
    out[dim] = lax.rem(out[dim] + by + 4, 4)
    return tuple(out)


def bulk(ref, send_sem, recv_sem, seq, tp):
    return pltpu.make_async_remote_copy(
        src_ref=ref, dst_ref=ref, send_sem=send_sem, recv_sem=recv_sem,
        device_id=(seq, 1 - tp), device_id_type=MESH,
    )


class Gather:
    ORDERS = ((2, 1, 0), (1, 0, 2), (0, 2, 1))

    def __init__(self, weights, send, recv, zyx, tp, seq):
        self.weights, self.send, self.recv, self.zyx, self.tp = weights, send, recv, zyx, tp
        self.seq = seq

    def bulk(self, ref, send, recv):
        return bulk(ref, self.send.at[send], self.recv.at[recv], self.seq, self.tp)

    def make(self, part, dim, step, index, columns, phase, sem):
        index = tuple(index)
        ref = self.weights.at[index[0], index[1], index[2], :, pl.ds(*columns)]
        return pltpu.make_async_remote_copy(
            src_ref=ref,
            dst_ref=ref,
            send_sem=self.send.at[phase],
            recv_sem=self.recv.at[sem],
            device_id=device(moved(self.zyx, dim, step), self.tp),
            device_id_type=MESH,
        )

    def own(self, part, which, incoming=False):
        dim = self.ORDERS[part][0]
        step = (1, -1, 2)[which]
        index = list(self.zyx)
        index[dim] = lax.rem(index[dim] - (step if incoming else 0) + 4, 4)
        return self.make(part, dim, step, index, (384 * part, 384), 0, 0)

    def copy(self, part, phase, sign, piece, forwarded=False, incoming=False, early=False):
        order = self.ORDERS[part]
        dim = order[phase]
        index = list(self.zyx)
        if phase == 2:
            index[order[0]] = pl.ds(0, 4)
        before = order[phase - 1]
        index[before] = lax.rem(self.zyx[before] + piece, 4)
        back = sign * ((1 if forwarded else 0) + (1 if incoming else 0))
        index[dim] = lax.rem(self.zyx[dim] - back + 4, 4)
        columns = (384 * part, 384)
        if phase == 2 and part < 2:
            columns = (384 * part + 256, 128) if early else (384 * part, 256)
        group = 2 if early else phase - 1
        sem = 33 + group
        if not forwarded and sign == (1 if piece < 2 else -1):
            sem = 1 + 12 * group + 4 * part + piece
        return self.make(part, dim, sign, index, columns, phase, sem)

    def start_own(self):
        for which in range(3):
            for part in range(3):
                self.own(part, which).start()

    def finish_own(self):
        self.bulk(self.weights.at[0, 0, pl.ds(0, 3)], 0, 0).wait_recv()

    def start(self, phase, pieces, parts=(0, 1, 2), early=False):
        for piece in pieces:
            for part in parts:
                for sign in (1, -1):
                    self.copy(part, phase, sign, piece, early=early).start()

    def forward(self, phase, pieces, parts=(0, 1, 2), early=False):
        for piece in pieces:
            sign = 1 if piece < 2 else -1
            for part in parts:
                self.copy(part, phase, sign, piece, incoming=True, early=early).wait_recv()
                self.copy(part, phase, sign, piece, forwarded=True, early=early).start()

    def finish(self, phase, early=False):
        if phase == 1:
            ref = self.weights.at[0, pl.ds(0, 2)]
        else:
            ref = self.weights.at[pl.ds(0, 2), :, :, :, pl.ds(0, 256 if early else 896)]
        self.bulk(ref, phase, 35 if early else 32 + phase).wait_recv()

    def drain(self):
        self.bulk(self.weights.at[0, 0, pl.ds(0, 3)], 0, 0).wait_send()
        self.bulk(self.weights.at[0, pl.ds(0, 3)], 1, 0).wait_send()
        self.bulk(self.weights.at[pl.ds(0, 3)], 2, 0).wait_send()


class Ring:
    PARTS = ((0, 48), (48, 96), (144, 112))
    ORDERS = ((2, 1, 0), (1, 0, 2), (0, 2, 1))

    def __init__(self, kv, extra, send, recv, zyx, tp, seq):
        self.kv, self.extra, self.send, self.recv = kv, extra, send, recv
        self.flat = kv.reshape(16, 4, 256, 256)
        self.zyx, self.tp, self.seq = zyx, tp, seq
        z, y, x = zyx
        self.row = 4 * z + y
        self.gives_extra = (x == 3) & (self.row < 7)
        self.takes_extra = (x == 0) & (self.row > 8)

    def base(self, source, target):
        later = (target - source + 3) // 4
        return jnp.maximum(self.zyx[0] - 2 + later, 0)

    def block(self, part, phase, at, kind):
        z, y, x = self.zyx
        tokens = pl.ds(*self.PARTS[part])
        half = (0, 1, 0, 1, 0, 1)[kind]
        if phase == 0:
            index = [z, y, x]
            index[self.ORDERS[part][0]] = at
            return self.kv.at[index[0], index[1], index[2], tokens]
        if part == 0:
            two = pl.ds(2 * half, 2)
            if phase == 1:
                return self.kv.at[z, at, two, tokens]
            return self.kv.at[at, two, :, tokens]
        if part == 1:
            if phase == 1:
                return self.kv.at[at, pl.ds(2 * half, 2), x, tokens]
            base = jnp.maximum(self.row - 8, 0)
            return self.flat.at[pl.ds(base + 5 * half, 5 - half), at, tokens]
        if phase == 1:
            base = jnp.maximum(z - 2, 0)
            return self.kv.at[pl.ds(base + 2 * half, 2 - half), y, at, tokens]
        raise NotImplementedError

    def copy(self, part, phase, kind, incoming=False):
        dim = self.ORDERS[part][phase]
        me = self.zyx[dim]
        sign = 1 if kind < 3 else -1
        back = 1 if kind in (2, 5) else 0
        if phase == 0 and kind == 2:
            sign, back = 2, 0
        at = lax.rem(me - sign * (back + (1 if incoming else 0)) + 4, 4)
        if part == 2 and phase == 2:
            to = me if incoming else lax.rem(me + sign + 4, 4)
            base = self.base(at, to)
            planes = pl.ds(base, 2)
            if back:
                planes = pl.ds(base + (1 if kind == 2 else 0), 1)
            ref = self.kv.at[planes, at, :, pl.ds(*self.PARTS[2])]
        else:
            ref = self.block(part, phase, at, kind)
        if phase == 0:
            sends, sem = 0, 0
        elif phase == 1:
            sends, sem = 1 + part, 7 + part
            if kind in (0, 3):
                sem = 1 + 2 * part + kind // 3
        else:
            sends, sem = 4 + part, 10 + 6 * part + kind
        return pltpu.make_async_remote_copy(
            src_ref=ref,
            dst_ref=ref,
            send_sem=self.send.at[sends],
            recv_sem=self.recv.at[sem],
            device_id=device(moved(self.zyx, dim, sign), self.tp),
            device_id_type=MESH,
        )

    def own_kinds(self, part, phase):
        if phase == 0:
            return (0, 3, 2)
        if (part, phase) == (2, 2):
            return (0, 3)
        if (part, phase) == (0, 2):
            return (0, 3, 1)
        return (0, 3, 1, 4)

    def sent_on(self, phase):
        return () if phase == 0 else (2, 5)

    def start(self, phase):
        for place in range(4):
            for part in range(3):
                kinds = self.own_kinds(part, phase)
                if place < len(kinds):
                    self.copy(part, phase, kinds[place]).start()
        if phase == 2:

            @pl.when(self.gives_extra)
            def _():
                self.extra_copy(False).start()

    def wait(self, *which):
        for part, phase, kind in which:
            self.copy(part, phase, kind, True).wait_recv()

    def forward(self, phase, parts=(0, 1, 2)):
        for kind in self.sent_on(phase):
            for part in parts:
                self.wait((part, phase, kind - 2))
                self.copy(part, phase, kind).start()

    def bulk(self, rows, cols, part, send, recv):
        tokens = pl.ds(0, 256 if part is None else self.PARTS[part][1])
        ref = self.flat.at[pl.ds(0, rows), pl.ds(0, cols), tokens]
        return bulk(ref, self.send.at[send], self.recv.at[recv], self.seq, self.tp)

    def finish(self, phase):
        if phase == 0:
            self.bulk(1, 3, None, 0, 0).wait_recv()
            return
        for part in range(3):
            self.bulk(2, 3 if part == 2 else 4, part, 1 + part, 7 + part).wait_recv()

    def drain(self):
        self.bulk(1, 3, None, 0, 0).wait_send()
        for part, (rows, cols) in enumerate(((3, 4), (3, 4), (3, 3))):
            self.bulk(rows, cols, part, 1 + part, 0).wait_send()
        for part, (rows, cols) in enumerate(((10, 4), (9, 3), (6, 4))):
            self.bulk(rows, cols, part, 4 + part, 0).wait_send()

        @pl.when(self.gives_extra)
        def _():
            self.extra_copy(False).wait_send()

    def extra_copy(self, incoming):
        z, y, x = self.zyx
        other = (self.seq + 64 - WINDOW if incoming else self.seq + WINDOW) % 64
        return pltpu.make_async_remote_copy(
            src_ref=self.kv.at[z, y, x],
            dst_ref=self.extra,
            send_sem=self.send.at[7],
            recv_sem=self.recv.at[28],
            device_id=(other, self.tp),
            device_id_type=MESH,
        )

    def greet(self, barrier):
        @pl.when(self.takes_extra)
        def _():
            pl.semaphore_signal(
                barrier, inc=1, device_id=(self.seq - WINDOW, self.tp), device_id_type=MESH
            )

    def greeted(self, barrier, partners):
        @pl.when(self.gives_extra)
        def _():
            pl.semaphore_wait(barrier, partners + 1)

        @pl.when(jnp.logical_not(self.gives_extra))
        def _():
            pl.semaphore_wait(barrier, partners)

    def shard(self, part, row, col):
        begin, size = self.PARTS[part]
        return (jnp.maximum(row, 0), col, begin), (row * 4 + col) * 256 + begin, size

    def row_keys(self, at):
        return [self.shard(1, self.row - 8 + r, at) for r in range(9)]

    def plane_keys(self, at):
        y = self.zyx[1]
        own = at is y
        base = jnp.maximum(self.zyx[0] - 2, 0) if own else self.base(at, y)
        planes = range(3 if own else 2)
        return [self.shard(2, (base + p) * 4 + at, col) for p in planes for col in range(4)]

    def before_keys(self):
        z = self.zyx[0]
        return [self.shard(0, 4 * z - 4 + r, col) for r in range(4) for col in range(4)]

    def edge_keys(self):
        y = self.zyx[1]
        rows = [self.row - 8 + r + 4 * ((y + r) // 4) for r in range(5)]
        return [self.shard(0, row, col) for row in rows for col in range(4)]

    def units(self):
        z, y, x = self.zyx
        left, right = lax.rem(x + 3, 4), lax.rem(x + 1, 4)
        below, above = lax.rem(y + 3, 4), lax.rem(y + 1, 4)
        before = self.before_keys()
        stream = self.row_keys(x) + self.plane_keys(y) + before[:8] + self.row_keys(left)
        stream += self.row_keys(right) + before[8:] + self.plane_keys(below)
        stream += self.plane_keys(above) + self.row_keys(lax.rem(x + 2, 4))
        stream += self.plane_keys(lax.rem(y + 2, 4)) + self.edge_keys()
        out, room = [[]], UNIT
        for (row, col, begin), at, size in stream:
            done = 0
            while done < size:
                if room == 0:
                    out.append([])
                    room = UNIT
                take = min(size - done, room)
                out[-1].append(((row, col, begin + done), at + done, take))
                done += take
                room -= take
        return out


def iota(shape, dim):
    return lax.broadcasted_iota(jnp.int32, shape, dim)


def to_column(row):
    n = row.shape[1]
    eye = iota((n, n), 0) == iota((n, n), 1)
    return jnp.sum(jnp.where(eye, jnp.broadcast_to(row, (n, n)), 0.0), axis=1, keepdims=True)


def to_row(column):
    n = column.shape[0]
    eye = iota((n, n), 0) == iota((n, n), 1)
    return jnp.sum(jnp.where(eye, jnp.broadcast_to(column, (n, n)), 0.0), axis=0, keepdims=True)


def one_hot(flag):
    return jnp.where(flag, 1.0, 0.0).astype(BF16)


def dot(a, b):
    return jnp.dot(a, b, preferred_element_type=F32)


def whole(
    patches, merge_up, merge_down, dest, slot, text, positions, documents, w_query, w_key, w_value,
    layer_out, attended_out,
    patch_v, up_v, down_v, text_v, pn, acc, disp, stage1, turned, stage2, part_f, part_s, part_r,
    merged, normed, weights, qkv, kv, extra, bounds, query, hold, top, unit_k, unit_v,
    load, send, recv, send1, recv1, send2, recv2, send3, recv3, kv_send, kv_recv,
):
    zyx, tp, seq = coords()
    z, y, x = zyx
    own = weights.at[z, y, x]
    def columns(source, begin, size, target, sem):
        return pltpu.make_async_copy(
            source.at[:, pl.ds(begin, size)], own.at[:, pl.ds(target, size)], load.at[sem]
        )

    loads = [
        columns(w_query, 0, 256, 0, 0),
        columns(w_key, 0, 128, 256, 1),
        columns(w_query, 256, 256, 384, 2),
        pltpu.make_async_copy(patches, patch_v, load.at[3]),
    ]
    own_loads = [columns(w_value, 0, 128, 640, 11), columns(w_query, 512, 384, 768, 12)]
    own_loads += loads[:3]

    def up_part(p):
        return pltpu.make_async_copy(
            merge_up.at[pl.ds(1280 * p, 1280)], up_v.at[p], load.at[4 + p]
        )

    loads += [up_part(p) for p in range(4)]
    loads.append(pltpu.make_async_copy(merge_down, down_v, load.at[8]))
    loads.append(pltpu.make_async_copy(text, text_v, load.at[9]))
    for copy in own_loads + loads[3:]:
        copy.start()

    barrier = pltpu.get_barrier_semaphore()
    partners = []
    for g in range(1, 16):
        partners.append(device(moved(moved(zyx, 0, g // 4), 1, g % 4), tp))
    for g in range(1, 4):
        partners.append(device(moved(zyx, 2, g), tp))
    partners.append((seq, 1 - tp))
    for partner in partners:
        pl.semaphore_signal(barrier, inc=1, device_id=partner, device_id_type=MESH)
    ring = Ring(kv, extra, kv_send, kv_recv, zyx, tp, seq)
    ring.greet(barrier)
    for copy in own_loads:
        copy.wait()
    loads[3].wait()
    rows = patch_v[...].astype(F32)
    scale = lax.rsqrt(jnp.mean(rows * rows, axis=1, keepdims=True) + EPS)
    scaled = (rows * scale).astype(BF16)
    o, i = iota((256, 256), 0), iota((256, 256), 1)
    pn[...] = dot(one_hot(i == 4 * (o % 64) + o // 64), scaled).astype(BF16)

    ring.greeted(barrier, len(partners))

    gather = Gather(weights, send, recv, zyx, tp, seq)
    gather.start_own()
    gather.start(1, (0,))

    loads[4].wait()
    acc[...] = dot(pn[0:64], up_v[0])
    gather.finish_own()
    gather.start(1, (3, 1, 2))

    def up_step(p, _):
        up_part(p).wait()
        acc[...] += dot(pn[pl.ds(pl.multiple_of(64 * p, 64), 64)], up_v[p])
        return 0

    lax.fori_loop(1, 4, up_step, 0)

    h = acc[...]
    hidden = (0.5 * h * (1.0 + lax.erf(h * 0.7071067811865476))).astype(BF16)

    dest_row = dest[...].astype(F32)
    dest_col = to_column(dest_row)
    before = (iota((64, 64), 0) < iota((64, 64), 1)) & (dest_col == dest_row)
    order = jnp.sum(jnp.where(before, 1.0, 0.0), axis=0, keepdims=True)
    place = dest_row * 2.0 + order
    chosen = one_hot(iota((128, 64), 0).astype(F32) == place)
    slot_col = to_column(slot[...].astype(F32)) + 1.0
    lane = iota((64, 128), 1)
    meta = jnp.where(lane == 0, slot_col, 0.0).astype(BF16)
    doc_col = to_column(documents[...].astype(F32))
    doc_lane = (iota((256, 128), 1) - 1).astype(F32)
    counts = jnp.sum(jnp.where(doc_col == doc_lane, 1.0, 0.0), axis=0, keepdims=True)
    routed = dot(chosen, hidden).astype(BF16)
    disp[:, :, 0:1280] = routed.reshape(16, 8, 1280)
    routed_meta = (dot(chosen, meta) + counts).astype(BF16)
    disp[:, :, 1280:1408] = routed_meta.reshape(16, 8, 128)

    me_g = z * 4 + y

    def first(g):
        far = moved(moved(zyx, 0, g // 4), 1, g % 4)
        at = far[0] * 4 + far[1]
        return pltpu.make_async_remote_copy(
            src_ref=disp.at[at],
            dst_ref=stage1.at[me_g],
            send_sem=send1.at[0],
            recv_sem=recv1.at[0],
            device_id=device(far, tp),
            device_id_type=MESH,
        )

    for g in range(1, 16):
        first(g).start()
    stage1[me_g] = disp[me_g]
    gather.forward(1, (0, 3, 1, 2))
    gather.start(2, (0,), (0, 1), True)
    gather.start(2, (0,))
    bulk(stage1.at[pl.ds(0, 15)], send1.at[0], recv1.at[0], seq, tp).wait_recv()
    o, i = iota((128, 128), 0), iota((128, 128), 1)
    turn = one_hot(i == ((o % 32) // 2) * 8 + (o // 32) * 2 + o % 2)
    turned[...] = dot(turn, stage1[...].reshape(128, 1408)).astype(BF16).reshape(4, 32, 1408)

    def second(g):
        far = moved(zyx, 2, g)
        return pltpu.make_async_remote_copy(
            src_ref=turned.at[far[2]],
            dst_ref=stage2.at[x],
            send_sem=send2.at[0],
            recv_sem=recv2.at[0],
            device_id=device(far, tp),
            device_id_type=MESH,
        )

    for g in range(1, 4):
        second(g).start()
    stage2[x] = turned[x]
    gather.forward(2, (0,), (0, 1), True)
    gather.finish(1)
    gather.start(2, (3, 2, 1), (0, 1), True)
    gather.start(2, (3, 2, 1), (2,))
    gather.start(2, (3,), (0, 1))
    gather.forward(2, (0,))
    bulk(stage2.at[pl.ds(0, 3)], send2.at[0], recv2.at[0], seq, tp).wait_recv()
    gather.forward(2, (3, 2, 1), (0, 1), True)
    gather.start(2, (2, 1), (0, 1))

    arrived = stage2[...].reshape(128, 1408)
    rows_in = arrived[:, 0:1280]
    meta_in = arrived[:, 1280:1408].astype(F32)
    loads[8].wait()

    def swap(piece):
        cols = pl.ds(896 * piece, 896)
        return pltpu.make_async_remote_copy(
            src_ref=part_s.at[:, cols],
            dst_ref=part_r.at[:, cols],
            send_sem=send3.at[0],
            recv_sem=recv3.at[piece],
            device_id=(seq, 1 - tp),
            device_id_type=MESH,
        )

    for piece in range(4):
        cols = slice(896 * piece, 896 * piece + 896)
        partial = dot(rows_in, down_v[:, cols])
        part_f[:, cols] = partial
        part_s[:, cols] = partial.astype(BF16)
        swap(piece).start()

    totals = jnp.sum(meta_in, axis=0, keepdims=True) * 0.5
    smaller = (doc_lane < doc_col) & (doc_lane >= 0.0)
    start_col = jnp.sum(jnp.where(smaller, totals, 0.0), axis=1, keepdims=True)
    total_col = to_column(totals)
    sub, lane = iota((128, 128), 0) - 1, iota((128, 128), 1)
    low = jnp.sum(jnp.where((sub >= 0) & (sub < lane), total_col, 0.0), axis=0, keepdims=True)
    high = jnp.sum(jnp.where((sub >= 0) & (sub <= lane), total_col, 0.0), axis=0, keepdims=True)
    lane = iota((1, 128), 1)
    shard_low = ((lane - 8) * 256).astype(F32)
    low = jnp.where(lane < 8, low, jnp.where(lane < 72, shard_low, -1e9))
    high = jnp.where(
        lane < 8, high, jnp.where(lane < 72, shard_low + 256.0, jnp.where(lane == 72, 0.0, -1e9))
    )
    bounds[0:1, :] = low
    bounds[1:2, :] = high

    slot_row = to_row(meta_in[:, 0:1])
    spot = (iota((256, 128), 0) + 1).astype(F32) == slot_row
    placed = one_hot(spot)
    hit = jnp.sum(jnp.where(spot, 1.0, 0.0), axis=1, keepdims=True) > 0.5
    loads[9].wait()
    squares = jnp.zeros((256, 1), F32)
    for piece in range(4):
        cols = slice(896 * piece, 896 * piece + 896)
        swap(piece).wait_recv()
        merged[...] = (part_f[:, cols] + part_r[:, cols].astype(F32)).astype(BF16)
        layer = jnp.where(hit, dot(placed, merged[...]), text_v[:, cols].astype(F32))
        text_v[:, cols] = layer.astype(BF16)
        squares += jnp.sum(layer * layer, axis=1, keepdims=True)
    out = pltpu.make_async_copy(
        text_v.at[:, pl.ds(pl.multiple_of(tp * 1792, 128), 1792)], layer_out, load.at[10]
    )
    out.start()
    factor = lax.rsqrt(squares * (1.0 / 3584.0) + EPS)
    for piece in range(4):
        cols = slice(896 * piece, 896 * piece + 896)
        normed[:, cols] = (text_v[:, cols].astype(F32) * factor).astype(BF16)

    pair = iota((256, 128), 1) % 64
    inverse = jnp.exp(pair.astype(F32) * (-2.0 / 128.0 * 13.815510557964274))
    at_t = to_column(positions[0:1, :].astype(F32))
    at_h = to_column(positions[1:2, :].astype(F32))
    at_w = to_column(positions[2:3, :].astype(F32))
    coord = jnp.where(pair < 16, at_t, jnp.where(pair < 40, at_h, at_w))
    angle = coord * inverse
    cosine = jnp.cos(angle)
    sine = jnp.sin(angle)
    sine = jnp.where(iota((256, 128), 1) < 64, -sine, sine)

    def rotated(v):
        return v * cosine + pltpu.roll(v, 64, 1) * sine

    def weight(begin, size):
        return weights[:, :, :, :, begin : begin + size].reshape(3584, size)

    gather.finish(2, True)
    pair = jnp.concatenate([weight(256, 128), weight(640, 128)], axis=1)
    qkv[:, 0:256] = dot(normed[...], pair)
    kv[z, y, x, :, 0:128] = rotated(qkv[:, 0:128]).astype(BF16)
    kv[z, y, x, :, 128:256] = qkv[:, 128:256].astype(BF16)
    ring.start(0)
    gather.forward(2, (3, 2, 1))
    wide = iota((256, 128), 1)
    shard = wide - 8
    hidden_doc = (wide < 8) & (wide.astype(F32) != doc_col)
    hidden_shard = (wide >= 8) & ((shard >= seq) | (shard < seq - WINDOW))
    veil = jnp.where(hidden_doc | hidden_shard, MASKED, 0.0).astype(BF16)
    for head in range(7):
        query[head, :, 128:256] = veil
    unit_v[:, 128:256] = jnp.ones((UNIT, 128), BF16)
    ring.finish(0)
    ring.start(1)
    ring.forward(1)
    gather.finish(2)
    for begin, size, head in ((0, 256, 0), (384, 256, 2), (768, 384, 4)):
        qkv[:, 0:size] = dot(normed[...], weight(begin, size))
        for part in range(size // 128):
            v = qkv[:, 128 * part : 128 * part + 128]
            query[head + part, :, 0:128] = rotated(v).astype(BF16)

    ones = jnp.ones((256, 128), BF16)
    keys = kv[z, y, x, :, 0:128]
    values = jnp.concatenate([kv[z, y, x, :, 128:256], ones], axis=1)
    key_at = (iota((256, 256), 1) + seq * 256).astype(F32)
    allowed = (iota((256, 256), 1) <= iota((256, 256), 0)) & (key_at >= start_col)
    for head in range(7):
        scores = lax.dot_general(
            query[head, :, 0:128], keys, (((1,), (1,)), ((), ())), preferred_element_type=F32
        )
        scores = jnp.where(allowed, scores, MASKED)
        peak = jnp.max(scores, axis=1, keepdims=True)
        top[head] = jnp.broadcast_to(peak, (256, 128))
        hold[head] = dot(jnp.exp2((scores - peak) * EXPONENT).astype(BF16), values)

    def attend(keys, values):
        def score(head):
            return lax.dot_general(
                query[head], keys, (((1,), (1,)), ((), ())), preferred_element_type=F32
            )

        scores = score(0)
        for head in range(7):
            following = score(head + 1) if head < 6 else None
            old = top[head]
            new = jnp.maximum(old, jnp.max(scores, axis=1, keepdims=True))
            probs = jnp.exp2((scores - new[:, 0:1]) * EXPONENT).astype(BF16)
            factor = jnp.exp2((old - new) * EXPONENT)
            top[head] = new
            sums = dot(probs, values)
            hold[head, :, 0:128] = hold[head, :, 0:128] * factor + sums[:, 0:128]
            hold[head, :, 128:256] = hold[head, :, 128:256] * factor + sums[:, 128:256]
            scores = following

    def marks(first_at, rows):
        at = (iota((rows, 128), 0) + first_at).astype(F32)
        return one_hot((at >= bounds[0:1, :]) & (at < bounds[1:2, :]))

    ring.finish(1)
    ring.start(2)

    def before_unit(number):
        if number == 1:
            ring.forward(2, (0, 1))
        elif number == 2:
            ring.wait((1, 2, 1), (1, 2, 4), (0, 2, 1))
            ring.forward(2, (2,))
        elif number == 4:
            ring.wait((1, 2, 2), (1, 2, 5), (2, 2, 2), (2, 2, 5))
        elif number == 5:
            ring.wait((0, 2, 2), (0, 2, 5))

    def fill(pieces):
        at = 0
        for (row, col, begin), first_at, rows in pieces:
            here = slice(at, at + rows)
            unit_k[here, 0:128] = ring.flat[row, col, begin : begin + rows, 0:128]
            unit_v[here, 0:128] = ring.flat[row, col, begin : begin + rows, 128:256]
            unit_k[here, 128:256] = marks(first_at, rows)
            at += rows

    units = ring.units()

    def from_extra(number):
        begin, at, rows = ((1120, 0, 64), (1344, 64, 192))[number - 4]
        here, there = slice(begin, begin + rows), slice(at, at + rows)
        unit_k[here, 0:128] = extra[there, 0:128]
        unit_v[here, 0:128] = extra[there, 128:256]
        unit_k[here, 128:256] = marks((seq - WINDOW) * 256 + at, rows)

    def unit(number, _):
        used = number < 0
        for which, pieces in enumerate(units):
            for _, first_at, _ in pieces:
                seen = (first_at >= (seq - WINDOW) * 256) & (first_at < seq * 256)
                used = used | ((number == which) & seen)

            @pl.when(number == which)
            def _():
                before_unit(which)
                fill(pieces)

        @pl.when(ring.takes_extra & (number == 4))
        def _():
            ring.extra_copy(True).wait_recv()
            from_extra(4)

        @pl.when(ring.takes_extra & (number == 5))
        def _():
            from_extra(5)

        @pl.when(used)
        def _():
            attend(unit_k[...], unit_v[...])

        return 0

    lax.fori_loop(0, len(units), unit, 0)

    for head in range(7):
        attended_out[:, 128 * head : 128 * head + 128] = (
            hold[head, :, 0:128] / hold[head, :, 128:256]
        ).astype(BF16)

    out.wait()
    gather.drain()
    ring.drain()
    bulk(stage1.at[pl.ds(0, 15)], send1.at[0], recv1.at[0], seq, tp).wait_send()
    bulk(stage2.at[pl.ds(0, 3)], send2.at[0], recv2.at[0], seq, tp).wait_send()
    bulk(part_s, send3.at[0], recv3.at[0], seq, tp).wait_send()


def hand_over(layer, attended, layer_out, attended_out, layer_v, attended_v, into, out):
    moves = []
    for n in range(4):
        moves.append((layer, layer_v, layer_out, pl.ds(64 * n, 64)))
    for n in range(2):
        moves.append((attended, attended_v, attended_out, pl.ds(128 * n, 128)))
    first = [
        pltpu.make_async_copy(a.at[rows], b.at[rows], into.at[n])
        for n, (a, b, _, rows) in enumerate(moves)
    ]
    then = [
        pltpu.make_async_copy(b.at[rows], c.at[rows], out.at[n])
        for n, (_, b, c, rows) in enumerate(moves)
    ]
    for copy in first:
        copy.start()
    for arrives, leaves in zip(first, then):
        arrives.wait()
        leaves.start()
    for copy in then:
        copy.wait()


def per_device(
    patches, merge_up, merge_down, dest, slot, text, positions, documents, w_query, w_key, w_value
):
    hbm = pl.BlockSpec(memory_space=pl.ANY)
    vmem = pl.BlockSpec(memory_space=pltpu.VMEM)
    dma = pltpu.SemaphoreType.DMA
    layer_part, attended = pl.pallas_call(
        whole,
        out_shape=(
            jax.ShapeDtypeStruct((256, 1792), BF16),
            jax.ShapeDtypeStruct((256, 896), BF16),
        ),
        in_specs=[hbm, hbm, hbm, vmem, vmem, hbm, vmem, vmem, hbm, hbm, hbm],
        out_specs=(hbm, vmem),
        scratch_shapes=[
            pltpu.VMEM((256, 1280), BF16),
            pltpu.VMEM((4, 1280, 1280), BF16),
            pltpu.VMEM((1280, 3584), BF16),
            pltpu.VMEM((256, 3584), BF16),
            pltpu.VMEM((256, 1280), BF16),
            pltpu.VMEM((64, 1280), F32),
            pltpu.VMEM((16, 8, 1408), BF16),
            pltpu.VMEM((16, 8, 1408), BF16),
            pltpu.VMEM((4, 32, 1408), BF16),
            pltpu.VMEM((4, 32, 1408), BF16),
            pltpu.VMEM((128, 3584), F32),
            pltpu.VMEM((128, 3584), BF16),
            pltpu.VMEM((128, 3584), BF16),
            pltpu.VMEM((128, 896), BF16),
            pltpu.VMEM((256, 3584), BF16),
            pltpu.VMEM((4, 4, 4, 56, 1152), BF16),
            pltpu.VMEM((256, 384), F32),
            pltpu.VMEM((4, 4, 4, 256, 256), BF16),
            pltpu.VMEM((256, 256), BF16),
            pltpu.VMEM((8, 128), F32),
            pltpu.VMEM((7, 256, 256), BF16),
            pltpu.VMEM((7, 256, 256), F32),
            pltpu.VMEM((7, 256, 128), F32),
            pltpu.VMEM((UNIT, 256), BF16),
            pltpu.VMEM((UNIT, 256), BF16),
            dma((13,)),
            dma((3,)),
            dma((36,)),
            dma((1,)),
            dma((1,)),
            dma((1,)),
            dma((1,)),
            dma((1,)),
            dma((4,)),
            dma((8,)),
            dma((29,)),
        ],
        compiler_params=pltpu.CompilerParams(
            collective_id=0, has_side_effects=True, vmem_limit_bytes=67043328
        ),
        name="whole",
    )(
        patches, merge_up, merge_down, dest.reshape(1, -1), slot.reshape(1, -1), text, positions,
        documents.reshape(1, -1), w_query, w_key, w_value,
    )
    return pl.pallas_call(
        hand_over,
        out_shape=(
            jax.ShapeDtypeStruct((256, 1792), BF16),
            jax.ShapeDtypeStruct((256, 896), BF16),
        ),
        in_specs=[hbm, hbm],
        out_specs=(hbm, hbm),
        scratch_shapes=[
            pltpu.VMEM((256, 1792), BF16),
            pltpu.VMEM((256, 896), BF16),
            dma((6,)),
            dma((6,)),
        ],
        name="hand_over",
    )(layer_part, attended)


def solution(mesh):
    in_specs = (
        P("seq", None),
        P(None, "tp"),
        P("tp", None),
        P("seq"),
        P("seq"),
        P("seq", None),
        P(None, "seq"),
        P("seq"),
        P("seq", "tp"),
        P("seq", "tp"),
        P("seq", "tp"),
    )
    out_specs = (P("seq", "tp"), P("seq", "tp"))
    return jax.shard_map(
        per_device, mesh=mesh, in_specs=in_specs, out_specs=out_specs, check_vma=False
    )
```
